32 devices in a mesh: dp: 4 (over y, z), ep: 8 (over x, core).
Axes of the slice: x: 4, y: 2, z: 2, core: 2. Of those that a mesh axis runs over, the one named last changes fastest.
The devices are a block of a 4x4x8 slice.
Arguments:
- x: bfloat16 [131072, 768], P(('dp', 'ep')), parts along dimension 0
- idx: int32 [131072, 1], P(('dp', 'ep')), parts along dimension 0
- w: float32 [131072, 1], P(('dp', 'ep')), parts along dimension 0
- slot: int32 [131072, 1], P(('dp', 'ep')), parts along dimension 0
- counts: int32 [32, 16], P(('dp', 'ep')), parts along dimension 0
- w1: bfloat16 [16, 768, 3072], P('ep')
- w3: bfloat16 [16, 768, 3072], P('ep')
- w2: bfloat16 [16, 3072, 768], P('ep')
Outputs:
- output: bfloat16 [131072, 768], P(('dp', 'ep')), parts along dimension 0
There are 4 independent parts. The reference program is written for one: setup_inputs(seed, part) draws one part's arguments, and reference() takes and returns one part's arrays. A program takes and returns all parts, laid end to end along the dimension named above; an argument that names none is the same for every part.
All inputs are finite; a program needn't handle non-finite values.
Results may differ from the reference program's by a relative error of at most 0.001.
Values are sent between devices in bfloat16 or wider.
A program may use at most 768 MiB of HBM per device.

```python
import jax
import jax.numpy as jnp
from jax import lax

GROUP = 8
TOK = 4096
D = 768
F = 3072
EXP_DEV = 2
TOPK = 1
E = EXP_DEV * GROUP
CAP = 4 * TOK * TOPK // E
HOT = max(1, E // 8)


def _route(key, hot):
    k1, k2 = jax.random.split(key)
    r = (1.0 + 2.0 * hot) * (0.8 + 0.4 * jax.random.uniform(k1, (E,), jnp.float32))
    q = r / jnp.sum(r)
    n = 1 + jnp.floor((TOK * TOPK - E) * q).astype(jnp.int32)
    n = n + (jnp.arange(E) < TOK * TOPK - jnp.sum(n)).astype(jnp.int32)
    seq = jnp.repeat(jnp.arange(E, dtype=jnp.int32), n, total_repeat_length=TOK * TOPK)
    off = jnp.arange(TOK * TOPK, dtype=jnp.int32) - (jnp.cumsum(n) - n)[seq]
    perm = jax.random.permutation(k2, TOK)
    return seq.reshape(TOPK, TOK).T[perm], off.reshape(TOPK, TOK).T[perm], n


def setup_inputs(seed: int = 0, part: int = 0) -> dict:
    kpart, kw = jax.random.split(jax.random.key(seed))
    kx, kr, kh, kg = jax.random.split(jax.random.fold_in(kpart, part), 4)
    k1, k3, k2 = jax.random.split(kw, 3)
    hot = (jax.random.permutation(kh, E) < HOT).astype(jnp.float32)
    idx, slot, counts = jax.vmap(_route, in_axes=(0, None))(jax.random.split(kr, GROUP), hot)
    x = jax.random.normal(kx, (GROUP * TOK, D), jnp.float32).astype(jnp.bfloat16)
    w = (0.5 + jax.random.uniform(kg, (GROUP * TOK, TOPK), jnp.float32)) / TOPK ** 0.5
    w1 = (jax.random.normal(k1, (E, D, F), jnp.float32) * D ** -0.5).astype(jnp.bfloat16)
    w3 = (jax.random.normal(k3, (E, D, F), jnp.float32) * D ** -0.5).astype(jnp.bfloat16)
    w2 = (jax.random.normal(k2, (E, F, D), jnp.float32) * F ** -0.5).astype(jnp.bfloat16)
    return dict(x=x, idx=idx.reshape(GROUP * TOK, TOPK), w=w, slot=slot.reshape(GROUP * TOK, TOPK),
                counts=counts, w1=w1, w3=w3, w2=w2)


def reference(x, idx, w, slot, counts, w1, w3, w2):
    t = x.shape[0]
    row = (jnp.arange(t) // TOK)[:, None] * CAP + slot
    xb = jnp.broadcast_to(x[:, None, :], (t, TOPK, D))
    buf = jnp.zeros((E, GROUP * CAP, D), x.dtype).at[idx, row].set(xb)
    live = (jnp.arange(CAP)[None, None, :] < counts.T[:, :, None]).reshape(E, GROUP * CAP)
    buf = jnp.where(live[:, :, None], buf, 0)

    def expert(a):
        r, a1, a3, a2 = a
        g = jnp.dot(r, a1, preferred_element_type=jnp.float32)
        u = jnp.dot(r, a3, preferred_element_type=jnp.float32)
        h = (jax.nn.silu(g) * u).astype(jnp.bfloat16)
        return jnp.dot(h, a2, preferred_element_type=jnp.float32).astype(jnp.bfloat16)

    y = lax.map(expert, (buf, w1, w3, w2))
    out = jnp.zeros((t, D), jnp.float32)
    for j in range(TOPK):
        out = out + w[:, j, None] * y[idx[:, j], row[:, j]].astype(jnp.float32)
    return out.astype(jnp.bfloat16)
```

```python
import functools

import jax
import jax.numpy as jnp
from jax import lax
from jax.experimental import pallas as pl
from jax.experimental.pallas import tpu as pltpu
from jax.sharding import PartitionSpec as P


ANY = pl.BlockSpec(memory_space=pl.ANY)
SMEM = pl.BlockSpec(memory_space=pltpu.SMEM)
VMEM = pl.BlockSpec(memory_space=pltpu.VMEM)
MESH = pl.DeviceIdType.MESH
ALIGN = 16
BIG = 64
VLIM = 66 * 10**6
CORES = 2


def _al(c):
    return (c + (ALIGN - 1)) // ALIGN * ALIGN


def _rows(op, src, s0, dst, d0, n, sem):
    def go(size, base):
        def body(i, _):
            s = pl.multiple_of(s0 + base + i * size, ALIGN)
            d = pl.multiple_of(d0 + base + i * size, ALIGN)
            cp = pltpu.make_async_copy(src.at[pl.ds(s, size)], dst.at[pl.ds(d, size)], sem)
            cp.start() if op == 0 else cp.wait()
            return 0
        return body
    nb = n // BIG
    lax.fori_loop(0, nb, go(BIG, 0), 0)
    lax.fori_loop(0, (n - nb * BIG) // ALIGN, go(ALIGN, nb * BIG), 0)


def _pack_kernel(nch, base, cnt, me, pos, x, *refs):
    own = refs[0]
    sb, so = refs[1:nch], refs[nch:2 * nch - 1]
    xs, os_, ob, sem = refs[2 * nch - 1:]
    tok, d = x.shape
    nl = d // 128
    ne = nch * (cnt.shape[0] // (nch * CORES) // nch)
    per = ne // nch
    chip = me[0]
    row = (chip * CORES + me[1]) * ne

    def widen(b, _):
        v = x[pl.ds(pl.multiple_of(b * 16, 16), 16), :].astype(jnp.float32)
        for h in range(2):
            for c in range(nl):
                xs[pl.ds(pl.multiple_of((b * 2 + h) * 8 * nl + c * 8, 8), 8), :] = v[h * 8:h * 8 + 8, c * 128:c * 128 + 128]
        return 0
    lax.fori_loop(0, tok // 16, widen, 0, unroll=2)

    def move(g, _):
        for u in range(16):
            src = g * (16 * nl) + (u // 8) * (8 * nl) + u % 8
            os_[pl.ds(pos[g * 16 + u], nl, stride=8), :] = xs[pl.ds(src, nl, stride=8), :]
        return 0
    lax.fori_loop(0, tok // 16, move, 0)

    sizes = []
    for j in range(nch):
        t = 0
        for q in range(per):
            t = t + _al(cnt[row + j * per + q])
        sizes.append(t)
    total = sum(sizes)

    def narrow(b, _):
        halves = []
        for h in range(2):
            halves.append(jnp.concatenate(
                [os_[pl.ds(pl.multiple_of((b * 2 + h) * 8 * nl + c * 8, 8), 8), :] for c in range(nl)], axis=1))
        ob[pl.ds(pl.multiple_of(b * 16, 16), 16), :] = jnp.concatenate(halves, axis=0).astype(jnp.bfloat16)
        return 0
    lax.fori_loop(0, total // 16, narrow, 0)

    for op in (0, 1):
        start = 0
        for j in range(nch):
            t = sizes[j]
            k = (j - chip + nch) % nch
            n1 = jnp.minimum(t, base)

            @pl.when(k == 0)
            def _(start=start, t=t):
                _rows(op, ob, start, own, 0, t, sem)
            for kk in range(1, nch):
                @pl.when(k == kk)
                def _(start=start, t=t, n1=n1, kk=kk):
                    _rows(op, ob, start, sb[kk - 1], 0, n1, sem)
                    _rows(op, ob, start + n1, so[kk - 1], 0, t - n1, sem)
            start = start + t


def _ffn_kernel(nch, base, roles, cnt, me, *refs):
    nr = sum(1 if k == 0 else 2 for k in roles)
    xin, refs = refs[:nr], refs[nr:]
    (wa1, wa3, wa2, wb1, wb3, wb2), refs = refs[:6], refs[6:]
    yout, refs = refs[:nr], refs[nr:]
    xb, v1, v3, v2, hs, wsem, xsem, ysem = refs
    el, d, f = wa1.shape
    per = CORES * el
    ne = nch * per
    chip, core = me[0], me[1]
    place = []
    at = 0
    for k in roles:
        place.append(at)
        at += 1 if k == 0 else 2

    def seg(q, k):
        dev = ((chip - k + nch) % nch) * CORES + core
        first = dev * ne + chip * per
        off = 0
        for p in range(per):
            off = off + jnp.where(p < q, _al(cnt[first + p]), 0)
        return off, _al(cnt[first + q])

    def total(q):
        return sum(seg(q, k)[1] for k in roles)

    def rows(op, q, out):
        slot = lax.rem(q, 2)
        buf = xb.at[slot]
        at = 0
        for k, p in zip(roles, place):
            off, n = seg(q, k)
            n1 = n if k == 0 else jnp.clip(base - off, 0, n)
            pieces = [(p, off, at, n1)]
            if k != 0:
                pieces.append((p + 1, jnp.maximum(off - base, 0), at + n1, n - n1))
            for r, there, here, m in pieces:
                if out:
                    _rows(op, buf, here, yout[r], there, m, ysem.at[slot])
                else:
                    _rows(op, xin[r], there, buf, here, m, xsem.at[slot])
            at = at + n

    def weights(op, q):
        slot = lax.rem(q, 2)
        mine = lax.div(q, el) == core
        i = lax.rem(q, el)

        def go(srcs):
            for n, (s, v) in enumerate(zip(srcs, (v1, v3, v2))):
                cp = pltpu.make_async_copy(s.at[i], v.at[slot], wsem.at[slot, n])
                cp.start() if op == 0 else cp.wait()
        if op == 1:
            go((wa1, wa3, wa2))
        else:
            pl.when(mine)(lambda: go((wa1, wa3, wa2)))
            pl.when(jnp.logical_not(mine))(lambda: go((wb1, wb3, wb2)))

    def tile(slot, r0, tm):
        r0 = pl.multiple_of(r0, 128)
        fc = min(512, f)
        xt = xb[slot, pl.ds(r0, tm), :]
        for j in range(f // fc):
            a = jnp.dot(xt, v1[slot, :, j * fc:(j + 1) * fc], preferred_element_type=jnp.float32)
            b = jnp.dot(xt, v3[slot, :, j * fc:(j + 1) * fc], preferred_element_type=jnp.float32)
            hs[:tm, j * fc:(j + 1) * fc] = (jax.nn.silu(a) * b).astype(jnp.bfloat16)
        y = jnp.dot(hs[:tm, :], v2[slot], preferred_element_type=jnp.float32)
        xb[slot, pl.ds(r0, tm), :] = y.astype(jnp.bfloat16)

    weights(0, 0)
    rows(0, 0, False)

    def expert(q, _):
        slot = lax.rem(q, 2)

        @pl.when(q >= 1)
        def _():
            rows(1, q - 1, True)

        @pl.when(q + 1 < per)
        def _():
            weights(0, q + 1)
            rows(0, q + 1, False)
        weights(1, q)
        rows(1, q, False)
        n = total(q)
        nbig = n // 256

        def big(t, _):
            tile(slot, t * 256, 256)
            return 0
        rest = n - nbig * 256
        nbig = nbig + (rest > 128).astype(jnp.int32)
        lax.fori_loop(0, nbig, big, 0)

        @pl.when(jnp.logical_and(rest > 0, rest <= 128))
        def _():
            tile(slot, nbig * 256, 128)
        rows(0, q, True)
        return 0
    lax.fori_loop(0, per, expert, 0)
    rows(1, jnp.int32(per - 1), True)


def _unpack_kernel(nch, base, cnt, me, pos, w, own, *refs):
    zb, zo = refs[:nch - 1], refs[nch - 1:2 * nch - 2]
    out, zin, os_, xs, sem = refs[2 * nch - 2:]
    tok, d = out.shape
    nl = d // 128
    ne = nch * (cnt.shape[0] // (nch * CORES) // nch)
    per = ne // nch
    chip = me[0]
    row = (chip * CORES + me[1]) * ne
    for op in (0, 1):
        start = 0
        for j in range(nch):
            t = 0
            for q in range(per):
                t = t + _al(cnt[row + j * per + q])
            k = (j - chip + nch) % nch
            n1 = jnp.minimum(t, base)

            @pl.when(k == 0)
            def _(start=start, t=t):
                _rows(op, own, 0, zin, start, t, sem)
            for kk in range(1, nch):
                @pl.when(k == kk)
                def _(start=start, t=t, n1=n1, kk=kk):
                    _rows(op, zb[kk - 1], 0, zin, start, n1, sem)
                    _rows(op, zo[kk - 1], 0, zin, start + n1, t - n1, sem)
            start = start + t

    def widen(b, _):
        v = zin[pl.ds(pl.multiple_of(b * 16, 16), 16), :].astype(jnp.float32)
        for h in range(2):
            for c in range(nl):
                os_[pl.ds(pl.multiple_of((b * 2 + h) * 8 * nl + c * 8, 8), 8), :] = v[h * 8:h * 8 + 8, c * 128:c * 128 + 128]
        return 0
    lax.fori_loop(0, start // 16, widen, 0)

    def move(g, _):
        for u in range(16):
            dst = g * (16 * nl) + (u // 8) * (8 * nl) + u % 8
            xs[pl.ds(dst, nl, stride=8), :] = os_[pl.ds(pos[g * 16 + u], nl, stride=8), :] * w[g * 16 + u]
        return 0
    lax.fori_loop(0, tok // 16, move, 0)

    def narrow(b, _):
        halves = []
        for h in range(2):
            halves.append(jnp.concatenate(
                [xs[pl.ds(pl.multiple_of((b * 2 + h) * 8 * nl + c * 8, 8), 8), :] for c in range(nl)], axis=1))
        out[pl.ds(pl.multiple_of(b * 16, 16), 16), :] = jnp.concatenate(halves, axis=0).astype(jnp.bfloat16)
        return 0
    lax.fori_loop(0, tok // 16, narrow, 0, unroll=2)


def _over_kernel(nch, sizes, back, *refs):
    src, dst, (ssem, rsem) = refs[:nch - 1], refs[nch - 1:2 * nch - 2], refs[2 * nch - 2:]
    ep = lax.axis_index('ep')
    chip, core = lax.div(ep, CORES), lax.rem(ep, CORES)
    barrier = pltpu.get_barrier_semaphore()
    for k in range(1, nch):
        pl.semaphore_signal(barrier, inc=1, device_id={'ep': lax.rem(chip + k, nch) * CORES + core}, device_id_type=MESH)
    pl.semaphore_wait(barrier, nch - 1)

    for me in range(nch):
        @pl.when(chip == me)
        def _(me=me):
            def copy(k, n, peer):
                return pltpu.make_async_remote_copy(
                    src_ref=src[k - 1].at[pl.ds(0, n)], dst_ref=dst[k - 1].at[pl.ds(0, n)],
                    send_sem=ssem.at[k - 1], recv_sem=rsem.at[k - 1],
                    device_id={'ep': peer * CORES + core}, device_id_type=MESH)
            sends, recvs = [], []
            for k in range(1, nch):
                there, before = (me + k) % nch, (me - k) % nch
                if back:
                    if sizes[me]:
                        sends.append(copy(k, sizes[me], before))
                    if sizes[there]:
                        recvs.append(copy(k, sizes[there], there))
                else:
                    if sizes[there]:
                        sends.append(copy(k, sizes[there], there))
                    if sizes[me]:
                        recvs.append(copy(k, sizes[me], before))
            for cp in sends:
                cp.start()
            for cp in sends:
                cp.wait_send()
            for cp in recvs:
                cp.wait_recv()


def _nothing_kernel(*refs):
    pass


def _cases(nch, steps, full):
    cases = [tuple([0] * nch)]
    for s in steps:
        for j in range(nch):
            cases.append(tuple(s if i == j else 0 for i in range(nch)))
    for j in range(nch):
        for l in range(j + 1, nch):
            cases.append(tuple(steps[0] if i in (j, l) else 0 for i in range(nch)))
    for s in steps:
        cases.append(tuple([s] * nch))
    cases.append(tuple([full] * nch))
    return cases


def solution(mesh):
    g_ = mesh.shape['ep']
    tok_spec = P(('dp', 'ep'), None)
    w_spec = P('ep', None, None)
    nch = g_ // CORES

    def local(x, idx, w, slot, counts, w1, w3, w2):
        tok, d = x.shape
        el, _, f = w1.shape
        per = CORES * el
        ne = g_ * el
        nl = d // 128
        base = tok // nch
        region = tok + ALIGN * per
        over = region - base
        steps = (tok * 7 // 64, tok * 13 // 64)
        cases = _cases(nch, steps, over)
        bf, i32 = jnp.bfloat16, jnp.int32
        ep = lax.axis_index('ep')
        me = jnp.stack([ep // CORES, ep % CORES]).astype(i32)

        cnt = lax.all_gather(counts[0], 'ep')
        aligned = _al(cnt).reshape(g_, nch, per).sum(-1).max(0)
        lv = sum((aligned > base + s).astype(i32) for s in (0,) + steps)
        lv = [lv[j] for j in range(nch)]
        worst = functools.reduce(jnp.maximum, lv)
        code = sum(lv[j] * (len(steps) + 2) ** j for j in range(nch))
        case = len(cases) - 1 - (len(steps) + 1 - jnp.maximum(worst, 1))
        for n, c in enumerate(cases[:-len(steps) - 1]):
            known = sum((steps.index(v) + 1 if v else 0) * (len(steps) + 2) ** j for j, v in enumerate(c))
            case = jnp.where(code == known, n, case)
        cnt = cnt.reshape(-1)

        own_al = _al(counts[0])
        first = jnp.sum(jnp.where(jnp.arange(ne)[None, :] < jnp.arange(ne)[:, None], own_al[None, :], 0), axis=1)
        e = idx.reshape(tok)
        row = slot.reshape(tok) + jnp.sum(
            jnp.where(e[None, :] == jnp.arange(ne)[:, None], first[:, None], 0), axis=0)
        pos = (row // 8) * (8 * nl) + row % 8
        wt = w.reshape(tok)

        rows = tok + ALIGN * ne
        params = pltpu.CompilerParams(vmem_limit_bytes=VLIM)
        sds = jax.ShapeDtypeStruct
        packed = pl.pallas_call(
            functools.partial(_pack_kernel, nch, base),
            out_shape=[sds((region, d), bf)] + [sds((base, d), bf)] * (nch - 1) + [sds((over, d), bf)] * (nch - 1),
            in_specs=[SMEM, SMEM, SMEM, VMEM], out_specs=[ANY] * (2 * nch - 1),
            scratch_shapes=[pltpu.VMEM((tok * nl, 128), jnp.float32), pltpu.VMEM((rows * nl, 128), jnp.float32),
                            pltpu.VMEM((rows, d), bf), pltpu.SemaphoreType.DMA],
            compiler_params=params, name='pack',
            cost_estimate=pl.CostEstimate(flops=2 * 10**9, bytes_accessed=3 * tok * d * 2, transcendentals=0),
        )(cnt, me, pos, x)
        own, sb, so = packed[0], packed[1:nch], packed[nch:]

        swap = [(2 * s + c, 2 * s + 1 - c) for s in range(nch) for c in range(CORES)]
        wp = [lax.ppermute(a, 'ep', swap) for a in (w1, w3, w2)]

        def shift(a, k):
            return lax.ppermute(a, 'ep', [(CORES * s + c, CORES * ((s + k) % nch) + c)
                                          for s in range(nch) for c in range(CORES)])

        def over_call(sizes, back, args):
            if not any(sizes):
                return pl.pallas_call(_nothing_kernel, out_shape=[sds((over, d), bf)] * (nch - 1),
                                      in_specs=[ANY] * (nch - 1), out_specs=[ANY] * (nch - 1), name='nothing')(*args)
            return pl.pallas_call(
                functools.partial(_over_kernel, nch, sizes, back),
                out_shape=[sds((over, d), bf)] * (nch - 1),
                in_specs=[ANY] * (nch - 1), out_specs=[ANY] * (nch - 1),
                scratch_shapes=[pltpu.SemaphoreType.DMA((nch - 1,)), pltpu.SemaphoreType.DMA((nch - 1,))],
                compiler_params=pltpu.CompilerParams(collective_id=1 if back else 0, has_side_effects=True),
                name='over_back' if back else 'over',
            )(*args)

        def exchange(back, args):
            return lax.switch(case, [functools.partial(lambda s, *a: tuple(over_call(s, back, a)), s) for s in cases], *args)

        xbs = [shift(sb[k - 1], k) for k in range(1, nch)]
        xo = exchange(False, so)

        def ffn(roles, xin):
            nr = len(xin)
            outs = [sds(a.shape, bf) for a in xin]
            xr = len(roles) * tok // 4 + 256
            n = tok * len(roles) // nch
            return pl.pallas_call(
                functools.partial(_ffn_kernel, nch, base, roles),
                out_shape=outs,
                in_specs=[SMEM, SMEM] + [ANY] * (nr + 6), out_specs=[ANY] * nr,
                scratch_shapes=[pltpu.VMEM((2, xr, d), bf), pltpu.VMEM((2, d, f), bf), pltpu.VMEM((2, d, f), bf),
                                pltpu.VMEM((2, f, d), bf), pltpu.VMEM((256, f), bf),
                                pltpu.SemaphoreType.DMA((2, 3)), pltpu.SemaphoreType.DMA((2,)),
                                pltpu.SemaphoreType.DMA((2,))],
                compiler_params=params, name='ffn_' + '_'.join(map(str, roles)),
                cost_estimate=pl.CostEstimate(flops=6 * n * d * f, bytes_accessed=per * 3 * d * f * 2, transcendentals=0),
            )(cnt, me, *xin, w1, w3, w2, *wp)

        yb, yo = [None] * (nch - 1), [None] * (nch - 1)
        zb = [None] * (nch - 1)
        for k in (*range(1, nch, 2), *range(2, nch, 2)):
            yb[k - 1], yo[k - 1] = ffn((k,), [xbs[k - 1], xo[k - 1]])
            zb[k - 1] = shift(yb[k - 1], nch - k)
        zo = exchange(True, yo)
        yown, = ffn((0,), [own])

        return pl.pallas_call(
            functools.partial(_unpack_kernel, nch, base),
            out_shape=sds((tok, d), bf),
            in_specs=[SMEM] * 4 + [ANY] * (2 * nch - 1), out_specs=VMEM,
            scratch_shapes=[pltpu.VMEM((rows, d), bf), pltpu.VMEM((rows * nl, 128), jnp.float32),
                            pltpu.VMEM((tok * nl, 128), jnp.float32), pltpu.SemaphoreType.DMA],
            compiler_params=params, name='unpack',
        )(cnt, me, pos, wt, yown, *zb, *zo)

    return jax.shard_map(local, mesh=mesh, in_specs=(tok_spec,) * 5 + (w_spec,) * 3,
                         out_specs=tok_spec, check_vma=False)
```

```python
import functools

import jax
import jax.numpy as jnp
from jax import lax
from jax.experimental import pallas as pl
from jax.experimental.pallas import tpu as pltpu
from jax.sharding import PartitionSpec as P


ANY = pl.BlockSpec(memory_space=pltpu.HBM)
SMEM = pl.BlockSpec(memory_space=pltpu.SMEM)
VMEM = pl.BlockSpec(memory_space=pltpu.VMEM)
MESH = pl.DeviceIdType.MESH
ALIGN = 16
BIG = 64
VLIM = 66 * 10**6
CORES = 2


def _al(c):
    return (c + (ALIGN - 1)) // ALIGN * ALIGN


def _rows(op, src, s0, dst, d0, n, sem):
    def go(size, base):
        def body(i, _):
            s = pl.multiple_of(s0 + base + i * size, ALIGN)
            d = pl.multiple_of(d0 + base + i * size, ALIGN)
            cp = pltpu.make_async_copy(src.at[pl.ds(s, size)], dst.at[pl.ds(d, size)], sem)
            cp.start() if op == 0 else cp.wait()
            return 0
        return body
    nb = n // BIG
    lax.fori_loop(0, nb, go(BIG, 0), 0)
    lax.fori_loop(0, (n - nb * BIG) // ALIGN, go(ALIGN, nb * BIG), 0)


def _plan_kernel(nch, bases, steps, ncase, cnt, me, cntp, perm, first, case):
    g = nch * CORES
    ne = cnt.shape[0] // g
    per = ne // nch
    half = per // 2
    lb, hb = bases
    mine = (me[0] * CORES + me[1]) * ne
    level, light, at = [], 0, 0
    for j in range(nch):
        tot = [functools.reduce(lambda u, v: u + v, [cnt[s * ne + j * per + q] for s in range(g)]) for q in range(per)]
        rank = []
        for q in range(per):
            r = 0
            for p in range(per):
                if p != q:
                    r = r + ((tot[p] <= tot[q]) if p < q else (tot[p] < tot[q])).astype(jnp.int32)
            rank.append(r)
        order = []
        for r in range(per):
            o = 0
            for q in range(per):
                o = jnp.where(rank[q] == r, q, o)
            order.append(o)
            perm[j * per + r] = o
        sums = [0, 0]
        for s in range(g):
            al = []
            for r in range(per):
                c = cnt[s * ne + j * per + order[r]]
                cntp[s * ne + j * per + r] = c
                al.append(_al(c))
            for i in range(2):
                sums[i] = jnp.maximum(sums[i], functools.reduce(lambda u, v: u + v, al[i * half:(i + 1) * half]))
        light = jnp.maximum(light, sums[0])
        level.append(sum((sums[1] > hb + t).astype(jnp.int32) for t in (0,) + steps))
        for r in range(per):
            first[j * per + order[r]] = at
            at = at + _al(cnt[mine + j * per + order[r]])
    worst = functools.reduce(jnp.maximum, level)
    worst = jnp.where(light > lb, len(steps) + 1, worst)
    code = sum(level[j] * (len(steps) + 2) ** j for j in range(nch))
    code = jnp.where(light > lb, -1, code)
    pick = ncase - 1 - (len(steps) + 1 - jnp.maximum(worst, 1))
    for n, c in enumerate(_cases(nch, steps, 0)[:ncase - len(steps) - 1]):
        known = sum((steps.index(v) + 1 if v else 0) * (len(steps) + 2) ** j for j, v in enumerate(c))
        pick = jnp.where(code == known, n, pick)
    case[0] = pick


def _parts(row, cntp, j, per):
    al = [_al(cntp[row + j * per + r]) for r in range(per)]
    half = per // 2
    return sum(al[:half]), sum(al[half:])


def _pieces(bases, tl, th):
    l1, h1 = jnp.minimum(tl, bases[0]), jnp.minimum(th, bases[1])
    return [(0, 0, l1), (1, l1, tl - l1), (2, tl, h1), (3, tl + h1, th - h1)]


def _pack_kernel(nch, bases, cnt, me, pos, x, *refs):
    own, outs = refs[0], refs[1:1 + 4 * (nch - 1)]
    xs, os_, ob, sem = refs[1 + 4 * (nch - 1):]
    tok, d = x.shape
    nl = d // 128
    ne = cnt.shape[0] // (nch * CORES)
    per = ne // nch
    chip = me[0]
    row = (chip * CORES + me[1]) * ne

    def widen(b, _):
        v = x[pl.ds(pl.multiple_of(b * 16, 16), 16), :].astype(jnp.float32)
        for h in range(2):
            for c in range(nl):
                xs[pl.ds(pl.multiple_of((b * 2 + h) * 8 * nl + c * 8, 8), 8), :] = v[h * 8:h * 8 + 8, c * 128:c * 128 + 128]
        return 0
    lax.fori_loop(0, tok // 16, widen, 0, unroll=2)

    def move(g, _):
        for u in range(16):
            src = g * (16 * nl) + (u // 8) * (8 * nl) + u % 8
            os_[pl.ds(pos[g * 16 + u], nl, stride=8), :] = xs[pl.ds(src, nl, stride=8), :]
        return 0
    lax.fori_loop(0, tok // 16, move, 0)

    sizes = [_parts(row, cnt, j, per) for j in range(nch)]
    total = sum(tl + th for tl, th in sizes)

    def narrow(b, _):
        halves = []
        for h in range(2):
            halves.append(jnp.concatenate(
                [os_[pl.ds(pl.multiple_of((b * 2 + h) * 8 * nl + c * 8, 8), 8), :] for c in range(nl)], axis=1))
        ob[pl.ds(pl.multiple_of(b * 16, 16), 16), :] = jnp.concatenate(halves, axis=0).astype(jnp.bfloat16)
        return 0
    lax.fori_loop(0, total // 16, narrow, 0)

    for op in (0, 1):
        start = 0
        for j in range(nch):
            tl, th = sizes[j]
            k = (j - chip + nch) % nch

            @pl.when(k == 0)
            def _(start=start, t=tl + th):
                _rows(op, ob, start, own, 0, t, sem)
            for kk in range(1, nch):
                @pl.when(k == kk)
                def _(start=start, tl=tl, th=th, kk=kk):
                    for i, at, n in _pieces(bases, tl, th):
                        _rows(op, ob, start + at, outs[4 * (kk - 1) + i], 0, n, sem)
            start = start + tl + th


def _ffn_kernel(nch, base, roles, ranks, cnt, perm, me, *refs):
    nr = sum(1 if k == 0 else 2 for k in roles)
    xin, refs = refs[:nr], refs[nr:]
    (wa1, wa3, wa2, wb1, wb3, wb2), refs = refs[:6], refs[6:]
    yout, refs = refs[:nr], refs[nr:]
    xb, v1, v3, v2, hs, wsem, xsem, ysem = refs
    el, d, f = wa1.shape
    per = CORES * el
    ne = nch * per
    chip, core = me[0], me[1]
    place = []
    at = 0
    for k in roles:
        place.append(at)
        at += 1 if k == 0 else 2

    def seg(q, k):
        dev = ((chip - k + nch) % nch) * CORES + core
        first = dev * ne + chip * per + ranks[0]
        off = 0
        for p in range(len(ranks)):
            off = off + jnp.where(p < q, _al(cnt[first + p]), 0)
        return off, _al(cnt[first + q])

    def total(q):
        return sum(seg(q, k)[1] for k in roles)

    def rows(op, q, out):
        slot = lax.rem(q, 2)
        buf = xb.at[slot]
        at = 0
        for k, p in zip(roles, place):
            off, n = seg(q, k)
            n1 = n if k == 0 else jnp.clip(base - off, 0, n)
            pieces = [(p, off, at, n1)]
            if k != 0:
                pieces.append((p + 1, jnp.maximum(off - base, 0), at + n1, n - n1))
            for r, there, here, m in pieces:
                if out:
                    _rows(op, buf, here, yout[r], there, m, ysem.at[slot])
                else:
                    _rows(op, xin[r], there, buf, here, m, xsem.at[slot])
            at = at + n

    def weights(op, q):
        slot = lax.rem(q, 2)
        e = perm[chip * per + ranks[0] + q]
        mine = lax.div(e, el) == core
        i = lax.rem(e, el)

        def go(srcs):
            for n, (s, v) in enumerate(zip(srcs, (v1, v3, v2))):
                cp = pltpu.make_async_copy(s.at[i], v.at[slot], wsem.at[slot, n])
                cp.start() if op == 0 else cp.wait()
        if op == 1:
            go((wa1, wa3, wa2))
        else:
            pl.when(mine)(lambda: go((wa1, wa3, wa2)))
            pl.when(jnp.logical_not(mine))(lambda: go((wb1, wb3, wb2)))

    def tile(slot, r0, tm):
        r0 = pl.multiple_of(r0, 128)
        fc = min(512, f)
        xt = xb[slot, pl.ds(r0, tm), :]
        for j in range(f // fc):
            a = jnp.dot(xt, v1[slot, :, j * fc:(j + 1) * fc], preferred_element_type=jnp.float32)
            b = jnp.dot(xt, v3[slot, :, j * fc:(j + 1) * fc], preferred_element_type=jnp.float32)
            hs[:tm, j * fc:(j + 1) * fc] = (jax.nn.silu(a) * b).astype(jnp.bfloat16)
        y = jnp.dot(hs[:tm, :], v2[slot], preferred_element_type=jnp.float32)
        xb[slot, pl.ds(r0, tm), :] = y.astype(jnp.bfloat16)

    weights(0, 0)
    rows(0, 0, False)

    def expert(q, _):
        slot = lax.rem(q, 2)

        @pl.when(q >= 1)
        def _():
            rows(1, q - 1, True)

        @pl.when(q + 1 < len(ranks))
        def _():
            weights(0, q + 1)
            rows(0, q + 1, False)
        weights(1, q)
        rows(1, q, False)
        n = total(q)
        nbig = n // 256

        def big(t, _):
            tile(slot, t * 256, 256)
            return 0
        rest = n - nbig * 256
        nbig = nbig + (rest > 128).astype(jnp.int32)
        lax.fori_loop(0, nbig, big, 0)

        @pl.when(jnp.logical_and(rest > 0, rest <= 128))
        def _():
            tile(slot, nbig * 256, 128)
        rows(0, q, True)
        return 0
    lax.fori_loop(0, len(ranks), expert, 0)
    rows(1, jnp.int32(len(ranks) - 1), True)


def _unpack_kernel(nch, bases, cnt, me, pos, w, own, *refs):
    ins = refs[:4 * (nch - 1)]
    out, zin, os_, xs, sem = refs[4 * (nch - 1):]
    tok, d = out.shape
    nl = d // 128
    ne = cnt.shape[0] // (nch * CORES)
    per = ne // nch
    chip = me[0]
    row = (chip * CORES + me[1]) * ne
    for op in (0, 1):
        start = 0
        for j in range(nch):
            tl, th = _parts(row, cnt, j, per)
            k = (j - chip + nch) % nch

            @pl.when(k == 0)
            def _(start=start, t=tl + th):
                _rows(op, own, 0, zin, start, t, sem)
            for kk in range(1, nch):
                @pl.when(k == kk)
                def _(start=start, tl=tl, th=th, kk=kk):
                    for i, at, n in _pieces(bases, tl, th):
                        _rows(op, ins[4 * (kk - 1) + i], 0, zin, start + at, n, sem)
            start = start + tl + th

    def widen(b, _):
        v = zin[pl.ds(pl.multiple_of(b * 16, 16), 16), :].astype(jnp.float32)
        for h in range(2):
            for c in range(nl):
                os_[pl.ds(pl.multiple_of((b * 2 + h) * 8 * nl + c * 8, 8), 8), :] = v[h * 8:h * 8 + 8, c * 128:c * 128 + 128]
        return 0
    lax.fori_loop(0, start // 16, widen, 0)

    def move(g, _):
        for u in range(16):
            dst = g * (16 * nl) + (u // 8) * (8 * nl) + u % 8
            xs[pl.ds(dst, nl, stride=8), :] = os_[pl.ds(pos[g * 16 + u], nl, stride=8), :] * w[g * 16 + u]
        return 0
    lax.fori_loop(0, tok // 16, move, 0)

    def narrow(b, _):
        halves = []
        for h in range(2):
            halves.append(jnp.concatenate(
                [xs[pl.ds(pl.multiple_of((b * 2 + h) * 8 * nl + c * 8, 8), 8), :] for c in range(nl)], axis=1))
        out[pl.ds(pl.multiple_of(b * 16, 16), 16), :] = jnp.concatenate(halves, axis=0).astype(jnp.bfloat16)
        return 0
    lax.fori_loop(0, tok // 16, narrow, 0, unroll=2)


def _cut(n, parts=3):
    u = n // ALIGN
    ends = [u * (i + 1) // parts * ALIGN for i in range(parts)]
    return [(lo, hi - lo) for lo, hi in zip([0] + ends[:-1], ends) if hi > lo]


def _exchange_kernel(nch, streams, back, *refs):
    ns, nk = len(streams), nch - 1
    src = [refs[i * nk:(i + 1) * nk] for i in range(ns)]
    dst = [refs[(ns + i) * nk:(ns + i + 1) * nk] for i in range(ns)]
    stage = refs[2 * ns * nk:2 * ns * nk + ns]
    send, recv, staged, passed = refs[2 * ns * nk + ns:]
    ep = lax.axis_index('ep')
    chip, core = lax.div(ep, CORES), lax.rem(ep, CORES)
    barrier = pltpu.get_barrier_semaphore()
    for k in range(1, nch):
        pl.semaphore_signal(barrier, inc=1, device_id={'ep': lax.rem(chip + k, nch) * CORES + core}, device_id_type=MESH)
    pl.semaphore_wait(barrier, nch - 1)
    opp = nch // 2
    turn = 1 - 2 * core

    def ring(c):
        return lax.rem(c + nch, nch)

    def copy(s, d, cut, a, b, to):
        return pltpu.make_async_remote_copy(
            src_ref=s.at[pl.ds(*cut)], dst_ref=d.at[pl.ds(*cut)], send_sem=a, recv_sem=b,
            device_id={'ep': to * CORES + core}, device_id_type=MESH)

    def each(what):
        for i, sizes in enumerate(streams):
            n = max(sizes)
            if not n:
                continue

            def guard(s, o, i=i, sizes=sizes):
                c = s if back else o
                if all(sizes):
                    return lambda f: f()
                return pl.when(functools.reduce(jnp.logical_or, [c == j for j in range(nch) if sizes[j]]))
            what(i, n, guard)

    def first_hop(i, p, cut):
        return copy(src[i][opp - 1], stage[i], cut, send.at[i, opp, p], staged.at[i, p], ring(chip + turn))

    def second_hop(i, p, cut):
        return copy(stage[i], dst[i][opp - 1], cut, passed.at[i, p], recv.at[i, opp, p], ring(chip + turn))

    def near(i, k, n):
        return copy(src[i][k - 1], dst[i][k - 1], (0, n), send.at[i, k, 0], recv.at[i, k, 0],
                    ring(chip - k if back else chip + k))

    def start(i, n, guard):
        @guard(chip, ring(chip + opp))
        def _():
            for p, cut in enumerate(_cut(n)):
                first_hop(i, p, cut).start()
        for k in range(1, nch):
            if k != opp:
                @guard(chip, ring(chip + k))
                def _(k=k):
                    near(i, k, n).start()

    def relay(i, n, guard):
        @guard(ring(chip - turn), ring(chip + turn))
        def _():
            for p, cut in enumerate(_cut(n)):
                first_hop(i, p, cut).wait_recv()
                second_hop(i, p, cut).start()

    def finish(i, n, guard):
        @guard(chip, ring(chip + opp))
        def _():
            for p, cut in enumerate(_cut(n)):
                first_hop(i, p, cut).wait_send()

        @guard(ring(chip - turn), ring(chip + turn))
        def _():
            for p, cut in enumerate(_cut(n)):
                second_hop(i, p, cut).wait_send()

        @guard(ring(chip + opp), chip)
        def _():
            for p, cut in enumerate(_cut(n)):
                second_hop(i, p, cut).wait_recv()
        for k in range(1, nch):
            if k != opp:
                @guard(chip, ring(chip + k))
                def _(k=k):
                    near(i, k, n).wait_send()

                @guard(ring(chip + k if back else chip - k), chip)
                def _(k=k):
                    near(i, k, n).wait_recv()
    each(start)
    each(relay)
    each(finish)


def _cases(nch, steps, full):
    cases = [tuple([0] * nch)]
    for s in steps:
        for j in range(nch):
            cases.append(tuple(s if i == j else 0 for i in range(nch)))
    for j in range(nch):
        for l in range(j + 1, nch):
            cases.append(tuple(steps[0] if i in (j, l) else 0 for i in range(nch)))
    for s in steps:
        cases.append(tuple([s] * nch))
    cases.append(tuple([full] * nch))
    return cases


def solution(mesh):
    g_ = mesh.shape['ep']
    tok_spec = P(('dp', 'ep'), None)
    w_spec = P('ep', None, None)
    nch = g_ // CORES

    def local(x, idx, w, slot, counts, w1, w3, w2):
        tok, d = x.shape
        el, _, f = w1.shape
        per = CORES * el
        ne = g_ * el
        nl = d // 128
        half = per // 2 * (4 * tok // ne)
        bases = (_al(tok * 17 // 128), _al(tok * 17 // 128))
        lb, hb = bases
        steps = (_al(tok * 15 // 128), _al(tok * 7 // 32))
        lo, ho = half - lb, half - hb
        region = tok + ALIGN * per
        cases = _cases(nch, steps, ho)
        bf, i32 = jnp.bfloat16, jnp.int32
        nk = nch - 1
        ep = lax.axis_index('ep')
        me = jnp.stack([ep // CORES, ep % CORES]).astype(i32)
        sds = jax.ShapeDtypeStruct
        params = pltpu.CompilerParams(vmem_limit_bytes=VLIM)

        gathered = lax.all_gather(counts[0], 'ep').reshape(-1)
        cnt, perm, first, case = pl.pallas_call(
            functools.partial(_plan_kernel, nch, bases, steps, len(cases)),
            out_shape=[sds((g_ * ne,), i32), sds((ne,), i32), sds((ne,), i32), sds((1,), i32)],
            in_specs=[SMEM] * 2, out_specs=[SMEM] * 4, name='plan')(gathered, me)

        first, *wx = lax.optimization_barrier((first, w1, w3, w2))
        swap = [(2 * s + c, 2 * s + 1 - c) for s in range(nch) for c in range(CORES)]
        wp = [lax.ppermute(a, 'ep', swap) for a in wx]

        e = idx.reshape(tok)
        row = slot.reshape(tok) + jnp.sum(
            jnp.where(e[None, :] == jnp.arange(ne)[:, None], first[:, None], 0), axis=0)
        pos = (row // 8) * (8 * nl) + row % 8
        wt = w.reshape(tok)

        rows = tok + ALIGN * ne
        packed = pl.pallas_call(
            functools.partial(_pack_kernel, nch, bases),
            out_shape=[sds((region, d), bf)] + [sds((n, d), bf) for n in (lb, lo, hb, ho)] * nk,
            in_specs=[SMEM, SMEM, SMEM, VMEM], out_specs=[ANY] * (1 + 4 * nk),
            scratch_shapes=[pltpu.VMEM((tok * nl, 128), jnp.float32), pltpu.VMEM((rows * nl, 128), jnp.float32),
                            pltpu.VMEM((rows, d), bf), pltpu.SemaphoreType.DMA],
            compiler_params=params, name='pack',
            cost_estimate=pl.CostEstimate(flops=2 * 10**9, bytes_accessed=3 * tok * d * 2, transcendentals=0),
        )(cnt, me, pos, x)
        own = packed[0]
        slb, slo, shb, sho = [[packed[1 + 4 * k + i] for k in range(nk)] for i in range(4)]

        def shift(a, k):
            return lax.ppermute(a, 'ep', [(CORES * s + c, CORES * ((s + k) % nch) + c)
                                          for s in range(nch) for c in range(CORES)])

        def exchange(back, whole, args):
            def run(heavy, light, *a):
                streams = (tuple([whole] * nch), heavy, light)
                outs = [sds(v.shape, bf) for v in a]
                stages = [sds((max(max(z), ALIGN), d), bf) for z in streams]
                return tuple(pl.pallas_call(
                    functools.partial(_exchange_kernel, nch, streams, back),
                    out_shape=outs + stages, in_specs=[ANY] * len(a), out_specs=[ANY] * (len(a) + 3),
                    scratch_shapes=[pltpu.SemaphoreType.DMA((3, nch, 3)), pltpu.SemaphoreType.DMA((3, nch, 3)),
                                    pltpu.SemaphoreType.DMA((3, 3)), pltpu.SemaphoreType.DMA((3, 3))],
                    compiler_params=pltpu.CompilerParams(collective_id=1 if back else 0, has_side_effects=True),
                    name='back' if back else 'there')(*a)[:len(a)])
            branches = [functools.partial(run, c, tuple([lo if n == len(cases) - 1 else 0] * nch))
                        for n, c in enumerate(cases)]
            out = lax.switch(case[0], branches, *args)
            return out[:nk], out[nk:2 * nk], out[2 * nk:]

        def ffn(base, roles, ranks, xin):
            nr = len(xin)
            xr = len(roles) * (4 * tok // ne) + 256
            n = tok // nch * len(roles) * len(ranks) // per
            return pl.pallas_call(
                functools.partial(_ffn_kernel, nch, base, roles, ranks),
                out_shape=[sds(a.shape, bf) for a in xin],
                in_specs=[SMEM] * 3 + [ANY] * (nr + 6), out_specs=[ANY] * nr,
                scratch_shapes=[pltpu.VMEM((2, xr, d), bf), pltpu.VMEM((2, d, f), bf), pltpu.VMEM((2, d, f), bf),
                                pltpu.VMEM((2, f, d), bf), pltpu.VMEM((256, f), bf),
                                pltpu.SemaphoreType.DMA((2, 3)), pltpu.SemaphoreType.DMA((2,)),
                                pltpu.SemaphoreType.DMA((2,))],
                compiler_params=params, name='ffn_' + '_'.join(map(str, roles + ranks)),
                cost_estimate=pl.CostEstimate(flops=6 * n * d * f, bytes_accessed=per * 3 * d * f * 2, transcendentals=0),
            )(cnt, perm, me, *xin, w1, w3, w2, *wp)

        far = tuple(range(1, nch))
        light, heavy = tuple(range(per // 2)), tuple(range(per // 2, per))

        def pairs(a, b):
            return [v for p in zip(a, b) for v in p]

        xlb, xho, xlo = exchange(False, lb, [*slb, *sho, *slo])
        held = lax.optimization_barrier((*shb, *xlb))
        shb, xlb = held[:nk], held[nk:]
        xhb = [shift(shb[k], k + 1) for k in range(nk)]
        yl = ffn(lb, far, light, pairs(xlb, xlo))
        ylb, ylo = yl[::2], yl[1::2]
        own, *ylb = lax.optimization_barrier((own, *ylb))
        yown, = ffn(region, (0,), light + heavy, [own])
        zlb = [shift(ylb[k], nch - 1 - k) for k in range(nk)]
        held = lax.optimization_barrier((yown, *xhb))
        yown, xhb = held[0], held[1:]
        yh = ffn(hb, far, heavy, pairs(xhb, xho))
        yhb, yho = yh[::2], yh[1::2]
        zhb, zho, zlo = exchange(True, hb, [*yhb, *yho, *ylo])

        return pl.pallas_call(
            functools.partial(_unpack_kernel, nch, bases),
            out_shape=sds((tok, d), bf),
            in_specs=[SMEM] * 4 + [ANY] * (1 + 4 * nk), out_specs=VMEM,
            scratch_shapes=[pltpu.VMEM((rows, d), bf), pltpu.VMEM((rows * nl, 128), jnp.float32),
                            pltpu.VMEM((tok * nl, 128), jnp.float32), pltpu.SemaphoreType.DMA],
            compiler_params=params, name='unpack',
        )(cnt, me, pos, wt, yown, *[v for p in zip(zlb, zlo, zhb, zho) for v in p])

    return jax.shard_map(local, mesh=mesh, in_specs=(tok_spec,) * 5 + (w_spec,) * 3,
                         out_specs=tok_spec, check_vma=False)
```

```python
import functools

import jax
import jax.numpy as jnp
from jax import lax
from jax.experimental import pallas as pl
from jax.experimental.pallas import tpu as pltpu
from jax.sharding import PartitionSpec as P


ANY = pl.BlockSpec(memory_space=pltpu.HBM)
SMEM = pl.BlockSpec(memory_space=pltpu.SMEM)
VMEM = pl.BlockSpec(memory_space=pltpu.VMEM)
MESH = pl.DeviceIdType.MESH
ALIGN = 16
BIG = 64
VLIM = 66 * 10**6
CORES = 2
WCUT = 4


def _al(c):
    return (c + (ALIGN - 1)) // ALIGN * ALIGN


def _rows(op, src, s0, dst, d0, n, sem):
    def go(size, base):
        def body(i, _):
            s = pl.multiple_of(s0 + base + i * size, ALIGN)
            d = pl.multiple_of(d0 + base + i * size, ALIGN)
            cp = pltpu.make_async_copy(src.at[pl.ds(s, size)], dst.at[pl.ds(d, size)], sem)
            cp.start() if op == 0 else cp.wait()
            return 0
        return body
    nb = n // BIG
    lax.fori_loop(0, nb, go(BIG, 0), 0)
    lax.fori_loop(0, (n - nb * BIG) // ALIGN, go(ALIGN, nb * BIG), 0)


def _plan_kernel(nch, bases, steps, ncase, cnt, me, cntp, perm, first, case):
    g = nch * CORES
    ne = cnt.shape[0] // g
    per = ne // nch
    half = per // 2
    lb, hb = bases
    mine = (me[0] * CORES + me[1]) * ne
    level, light, at = [], 0, 0
    for j in range(nch):
        tot = [functools.reduce(lambda u, v: u + v, [cnt[s * ne + j * per + q] for s in range(g)]) for q in range(per)]
        rank = []
        for q in range(per):
            r = 0
            for p in range(per):
                if p != q:
                    r = r + ((tot[p] <= tot[q]) if p < q else (tot[p] < tot[q])).astype(jnp.int32)
            rank.append(r)
        order = []
        for r in range(per):
            o = 0
            for q in range(per):
                o = jnp.where(rank[q] == r, q, o)
            order.append(o)
            perm[j * per + r] = o
        sums = [0, 0]
        for s in range(g):
            al = []
            for r in range(per):
                c = cnt[s * ne + j * per + order[r]]
                cntp[s * ne + j * per + r] = c
                al.append(_al(c))
            for i in range(2):
                sums[i] = jnp.maximum(sums[i], functools.reduce(lambda u, v: u + v, al[i * half:(i + 1) * half]))
        light = jnp.maximum(light, sums[0])
        level.append(sum((sums[1] > hb + t).astype(jnp.int32) for t in (0,) + steps))
        for r in range(per):
            first[j * per + order[r]] = at
            at = at + _al(cnt[mine + j * per + order[r]])
    worst = functools.reduce(jnp.maximum, level)
    worst = jnp.where(light > lb, len(steps) + 1, worst)
    code = sum(level[j] * (len(steps) + 2) ** j for j in range(nch))
    code = jnp.where(light > lb, -1, code)
    pick = ncase - 1 - (len(steps) + 1 - jnp.maximum(worst, 1))
    for n, c in enumerate(_cases(nch, steps, 0)[:ncase - len(steps) - 1]):
        known = sum((steps.index(v) + 1 if v else 0) * (len(steps) + 2) ** j for j, v in enumerate(c))
        pick = jnp.where(code == known, n, pick)
    case[0] = pick


def _parts(row, cntp, j, per):
    al = [_al(cntp[row + j * per + r]) for r in range(per)]
    half = per // 2
    return sum(al[:half]), sum(al[half:])


def _pieces(bases, tl, th):
    l1, h1 = jnp.minimum(tl, bases[0]), jnp.minimum(th, bases[1])
    return [(0, 0, l1), (1, l1, tl - l1), (2, tl, h1), (3, tl + h1, th - h1)]


def _widen(src, dst, lo, hi):
    nl = src.shape[1] // 128

    def body(b, _):
        v = src[pl.ds(pl.multiple_of(b * 16, 16), 16), :].astype(jnp.float32)
        for h in range(2):
            for c in range(nl):
                dst[pl.ds(pl.multiple_of((b * 2 + h) * 8 * nl + c * 8, 8), 8), :] = \
                    v[h * 8:h * 8 + 8, c * 128:c * 128 + 128]
        return 0
    lax.fori_loop(lo, hi, body, 0)


def _narrow(src, dst, lo, hi):
    nl = dst.shape[1] // 128

    def body(b, _):
        halves = []
        for h in range(2):
            halves.append(jnp.concatenate(
                [src[pl.ds(pl.multiple_of((b * 2 + h) * 8 * nl + c * 8, 8), 8), :] for c in range(nl)], axis=1))
        dst[pl.ds(pl.multiple_of(b * 16, 16), 16), :] = jnp.concatenate(halves, axis=0).astype(jnp.bfloat16)
        return 0
    lax.fori_loop(lo, hi, body, 0)


CHUNKS = 8


def _pack_kernel(nch, bases, cnt, me, pos, x, *refs):
    outs = refs[:2 + 4 * (nch - 1)]
    xv, xs, os_, ob, sem, xsem = refs[2 + 4 * (nch - 1):]
    tok, d = x.shape
    nl = d // 128
    ne = cnt.shape[0] // (nch * CORES)
    per = ne // nch
    chip = me[0]
    row = (chip * CORES + me[1]) * ne
    step = tok // CHUNKS

    def fetch(c):
        return pltpu.make_async_copy(x.at[pl.ds(c * step, step)], xv.at[pl.ds(c * step, step)], xsem.at[c])
    for c in range(CHUNKS):
        fetch(c).start()

    def move(g, _):
        for u in range(16):
            src = g * (16 * nl) + (u // 8) * (8 * nl) + u % 8
            os_[pl.ds(pos[g * 16 + u], nl, stride=8), :] = xs[pl.ds(src, nl, stride=8), :]
        return 0
    for c in range(CHUNKS):
        fetch(c).wait()
        _widen(xv, xs, c * step // 16, (c + 1) * step // 16)
    lax.fori_loop(0, tok // 16, move, 0)

    for op in (0, 1):
        start = 0
        for j in range(nch):
            tl, th = _parts(row, cnt, j, per)
            k = (j - chip + nch) % nch
            if op == 0:
                _narrow(os_, ob, start // 16, (start + tl + th) // 16)

            @pl.when(k == 0)
            def _(start=start, tl=tl, th=th):
                _rows(op, ob, start, outs[0], 0, tl, sem)
                _rows(op, ob, start + tl, outs[1], 0, th, sem)
            for kk in range(1, nch):
                @pl.when(k == kk)
                def _(start=start, tl=tl, th=th, kk=kk):
                    for i, at, n in _pieces(bases, tl, th):
                        _rows(op, ob, start + at, outs[2 + 4 * (kk - 1) + i], 0, n, sem)
            start = start + tl + th


def _ffn_kernel(nch, base, roles, ranks, cnt, perm, me, *refs):
    nr = sum(1 if k == 0 else 2 for k in roles)
    xin, refs = refs[:nr], refs[nr:]
    (wa1, wa3, wa2, wb1, wb3, wb2), refs = refs[:6], refs[6:]
    yout, refs = refs[:nr], refs[nr:]
    xb, v1, v3, v2, hs, wsem, xsem, ysem = refs
    el, d, f = wa1.shape
    per = CORES * el
    ne = nch * per
    chip, core = me[0], me[1]
    place = []
    at = 0
    for k in roles:
        place.append(at)
        at += 1 if k == 0 else 2

    def seg(q, k):
        dev = ((chip - k + nch) % nch) * CORES + core
        first = dev * ne + chip * per + ranks[0]
        off = 0
        for p in range(len(ranks)):
            off = off + jnp.where(p < q, _al(cnt[first + p]), 0)
        return off, _al(cnt[first + q])

    def total(q):
        return sum(seg(q, k)[1] for k in roles)

    def rows(op, q, out):
        slot = lax.rem(q, 2)
        buf = xb.at[slot]
        at = 0
        for k, p in zip(roles, place):
            off, n = seg(q, k)
            n1 = n if k == 0 else jnp.clip(base - off, 0, n)
            pieces = [(p, off, at, n1)]
            if k != 0:
                pieces.append((p + 1, jnp.maximum(off - base, 0), at + n1, n - n1))
            for r, there, here, m in pieces:
                if out:
                    _rows(op, buf, here, yout[r], there, m, ysem.at[slot])
                else:
                    _rows(op, xin[r], there, buf, here, m, xsem.at[slot])
            at = at + n

    def weights(op, q):
        slot = lax.rem(q, 2)
        e = perm[chip * per + ranks[0] + q]
        mine = lax.div(e, el) == core
        i = lax.rem(e, el)

        def go(srcs):
            for n, (s, v) in enumerate(zip(srcs, (v1, v3, v2))):
                m = v.shape[1] // WCUT
                for c in range(WCUT):
                    cp = pltpu.make_async_copy(s.at[i, pl.ds(c * m, m)], v.at[slot, pl.ds(c * m, m)], wsem.at[slot, n])
                    cp.start() if op == 0 else cp.wait()
        if op == 1:
            go((wa1, wa3, wa2))
        else:
            pl.when(mine)(lambda: go((wa1, wa3, wa2)))
            pl.when(jnp.logical_not(mine))(lambda: go((wb1, wb3, wb2)))

    def tile(slot, r0, tm):
        r0 = pl.multiple_of(r0, 128)
        fc = min(512, f)
        xt = xb[slot, pl.ds(r0, tm), :]
        for j in range(f // fc):
            a = jnp.dot(xt, v1[slot, :, j * fc:(j + 1) * fc], preferred_element_type=jnp.float32)
            b = jnp.dot(xt, v3[slot, :, j * fc:(j + 1) * fc], preferred_element_type=jnp.float32)
            hs[:tm, j * fc:(j + 1) * fc] = (jax.nn.silu(a) * b).astype(jnp.bfloat16)
        y = jnp.dot(hs[:tm, :], v2[slot], preferred_element_type=jnp.float32)
        xb[slot, pl.ds(r0, tm), :] = y.astype(jnp.bfloat16)

    weights(0, 0)
    rows(0, 0, False)

    def expert(q, _):
        slot = lax.rem(q, 2)

        @pl.when(q >= 1)
        def _():
            rows(1, q - 1, True)

        @pl.when(q + 1 < len(ranks))
        def _():
            weights(0, q + 1)
            rows(0, q + 1, False)
        weights(1, q)
        rows(1, q, False)
        n = total(q)
        nbig = n // 256

        def big(t, _):
            tile(slot, t * 256, 256)
            return 0
        rest = n - nbig * 256
        nbig = nbig + (rest > 128).astype(jnp.int32)
        lax.fori_loop(0, nbig, big, 0)

        @pl.when(jnp.logical_and(rest > 0, rest <= 128))
        def _():
            tile(slot, nbig * 256, 128)
        rows(0, q, True)
        return 0
    lax.fori_loop(0, len(ranks), expert, 0)
    rows(1, jnp.int32(len(ranks) - 1), True)


def _unpack_kernel(nch, bases, cnt, me, pos, w, *refs):
    ins = refs[:2 + 4 * (nch - 1)]
    out, zin, os_, xs, ov, sem, osem = refs[2 + 4 * (nch - 1):]
    tok, d = out.shape
    nl = d // 128
    ne = cnt.shape[0] // (nch * CORES)
    per = ne // nch
    chip = me[0]
    row = (chip * CORES + me[1]) * ne
    for op in (0, 1):
        start = 0
        for j in range(nch):
            tl, th = _parts(row, cnt, j, per)
            k = (j - chip + nch) % nch

            @pl.when(k == 0)
            def _(start=start, tl=tl, th=th, j=j):
                _rows(op, ins[0], 0, zin, start, tl, sem.at[j])
                _rows(op, ins[1], 0, zin, start + tl, th, sem.at[j])
            for kk in range(1, nch):
                @pl.when(k == kk)
                def _(start=start, tl=tl, th=th, kk=kk, j=j):
                    for i, at, n in _pieces(bases, tl, th):
                        _rows(op, ins[2 + 4 * (kk - 1) + i], 0, zin, start + at, n, sem.at[j])
            if op == 1:
                _widen(zin, os_, start // 16, (start + tl + th) // 16)
            start = start + tl + th

    def move(g, _):
        for u in range(16):
            dst = g * (16 * nl) + (u // 8) * (8 * nl) + u % 8
            xs[pl.ds(dst, nl, stride=8), :] = os_[pl.ds(pos[g * 16 + u], nl, stride=8), :] * w[g * 16 + u]
        return 0
    step = tok // CHUNKS

    def put(c):
        return pltpu.make_async_copy(ov.at[pl.ds(c * step, step)], out.at[pl.ds(c * step, step)], osem.at[c])
    for c in range(CHUNKS):
        lo, hi = c * step // 16, (c + 1) * step // 16
        lax.fori_loop(lo, hi, move, 0)
        _narrow(xs, ov, lo, hi)
        put(c).start()
    for c in range(CHUNKS):
        put(c).wait()


def _cut(n, parts=3):
    u = n // ALIGN
    ends = [u * (i + 1) // parts * ALIGN for i in range(parts)]
    return [(lo, hi - lo) for lo, hi in zip([0] + ends[:-1], ends) if hi > lo]


def _exchange_kernel(nch, streams, back, *refs):
    ns, nk = len(streams), nch - 1
    src = [refs[i * nk:(i + 1) * nk] for i in range(ns)]
    dst = [refs[(ns + i) * nk:(ns + i + 1) * nk] for i in range(ns)]
    stage = refs[2 * ns * nk:2 * ns * nk + ns]
    send, recv, staged, passed = refs[2 * ns * nk + ns:]
    ep = lax.axis_index('ep')
    chip, core = lax.div(ep, CORES), lax.rem(ep, CORES)
    barrier = pltpu.get_barrier_semaphore()
    for k in range(1, nch):
        pl.semaphore_signal(barrier, inc=1, device_id={'ep': lax.rem(chip + k, nch) * CORES + core}, device_id_type=MESH)
    pl.semaphore_wait(barrier, nch - 1)
    opp = nch // 2
    turn = 1 - 2 * core

    def ring(c):
        return lax.rem(c + nch, nch)

    def copy(s, d, cut, a, b, to):
        return pltpu.make_async_remote_copy(
            src_ref=s.at[pl.ds(*cut)], dst_ref=d.at[pl.ds(*cut)], send_sem=a, recv_sem=b,
            device_id={'ep': to * CORES + core}, device_id_type=MESH)

    def each(what):
        for i, sizes in enumerate(streams):
            n = max(sizes)
            if not n:
                continue

            def guard(s, o, i=i, sizes=sizes):
                c = s if back else o
                if all(sizes):
                    return lambda f: f()
                return pl.when(functools.reduce(jnp.logical_or, [c == j for j in range(nch) if sizes[j]]))
            what(i, n, guard)

    def first_hop(i, p, cut):
        return copy(src[i][opp - 1], stage[i], cut, send.at[i, opp, p], staged.at[i, p], ring(chip + turn))

    def second_hop(i, p, cut):
        return copy(stage[i], dst[i][opp - 1], cut, passed.at[i, p], recv.at[i, opp, p], ring(chip + turn))

    def near(i, k, n):
        return copy(src[i][k - 1], dst[i][k - 1], (0, n), send.at[i, k, 0], recv.at[i, k, 0],
                    ring(chip - k if back else chip + k))

    def start(i, n, guard):
        @guard(chip, ring(chip + opp))
        def _():
            for p, cut in enumerate(_cut(n)):
                first_hop(i, p, cut).start()
        for k in range(1, nch):
            if k != opp:
                @guard(chip, ring(chip + k))
                def _(k=k):
                    near(i, k, n).start()

    def relay(i, n, guard):
        @guard(ring(chip - turn), ring(chip + turn))
        def _():
            for p, cut in enumerate(_cut(n)):
                first_hop(i, p, cut).wait_recv()
                second_hop(i, p, cut).start()

    def finish(i, n, guard):
        @guard(chip, ring(chip + opp))
        def _():
            for p, cut in enumerate(_cut(n)):
                first_hop(i, p, cut).wait_send()

        @guard(ring(chip - turn), ring(chip + turn))
        def _():
            for p, cut in enumerate(_cut(n)):
                second_hop(i, p, cut).wait_send()

        @guard(ring(chip + opp), chip)
        def _():
            for p, cut in enumerate(_cut(n)):
                second_hop(i, p, cut).wait_recv()
        for k in range(1, nch):
            if k != opp:
                @guard(chip, ring(chip + k))
                def _(k=k):
                    near(i, k, n).wait_send()

                @guard(ring(chip + k if back else chip - k), chip)
                def _(k=k):
                    near(i, k, n).wait_recv()
    each(start)
    each(relay)
    each(finish)


def _cases(nch, steps, full):
    cases = [tuple([0] * nch)]
    for s in steps:
        for j in range(nch):
            cases.append(tuple(s if i == j else 0 for i in range(nch)))
    for j in range(nch):
        for l in range(j + 1, nch):
            cases.append(tuple(steps[0] if i in (j, l) else 0 for i in range(nch)))
    for s in steps:
        cases.append(tuple([s] * nch))
    cases.append(tuple([full] * nch))
    return cases


def solution(mesh):
    g_ = mesh.shape['ep']
    tok_spec = P(('dp', 'ep'), None)
    w_spec = P('ep', None, None)
    nch = g_ // CORES

    def local(x, idx, w, slot, counts, w1, w3, w2):
        tok, d = x.shape
        el, _, f = w1.shape
        per = CORES * el
        ne = g_ * el
        nl = d // 128
        half = per // 2 * (4 * tok // ne)
        bases = (_al(tok * 17 // 128), _al(tok * 17 // 128))
        lb, hb = bases
        steps = (_al(tok * 15 // 128), _al(tok * 7 // 32))
        lo, ho = half - lb, half - hb
        cases = _cases(nch, steps, ho)
        bf, i32 = jnp.bfloat16, jnp.int32
        nk = nch - 1
        ep = lax.axis_index('ep')
        me = jnp.stack([ep // CORES, ep % CORES]).astype(i32)
        sds = jax.ShapeDtypeStruct
        params = pltpu.CompilerParams(vmem_limit_bytes=VLIM)

        gathered = lax.all_gather(counts[0], 'ep').reshape(-1)
        cnt, perm, first, case = pl.pallas_call(
            functools.partial(_plan_kernel, nch, bases, steps, len(cases)),
            out_shape=[sds((g_ * ne,), i32), sds((ne,), i32), sds((ne,), i32), sds((1,), i32)],
            in_specs=[SMEM] * 2, out_specs=[SMEM] * 4, name='plan')(gathered, me)

        first, *wx = lax.optimization_barrier((first, w1, w3, w2))
        swap = [(2 * s + c, 2 * s + 1 - c) for s in range(nch) for c in range(CORES)]
        wp = [lax.ppermute(a, 'ep', swap) for a in wx]

        e = idx.reshape(tok)
        row = slot.reshape(tok) + jnp.sum(
            jnp.where(e[None, :] == jnp.arange(ne)[:, None], first[:, None], 0), axis=0)
        pos = (row // 8) * (8 * nl) + row % 8
        wt = w.reshape(tok)

        rows = tok + ALIGN * ne
        packed = pl.pallas_call(
            functools.partial(_pack_kernel, nch, bases),
            out_shape=[sds((half, d), bf)] * 2 + [sds((n, d), bf) for n in (lb, lo, hb, ho)] * nk,
            in_specs=[SMEM, SMEM, SMEM, ANY], out_specs=[ANY] * (2 + 4 * nk),
            scratch_shapes=[pltpu.VMEM((tok, d), bf), pltpu.VMEM((tok * nl, 128), jnp.float32),
                            pltpu.VMEM((rows * nl, 128), jnp.float32), pltpu.VMEM((rows, d), bf),
                            pltpu.SemaphoreType.DMA, pltpu.SemaphoreType.DMA((CHUNKS,))],
            compiler_params=params, name='pack',
            cost_estimate=pl.CostEstimate(flops=2 * 10**9, bytes_accessed=3 * tok * d * 2, transcendentals=0),
        )(cnt, me, pos, x)
        ownl, ownh = packed[:2]
        slb, slo, shb, sho = [[packed[2 + 4 * k + i] for k in range(nk)] for i in range(4)]

        def shift(a, k):
            return lax.ppermute(a, 'ep', [(CORES * s + c, CORES * ((s + k) % nch) + c)
                                          for s in range(nch) for c in range(CORES)])

        def exchange(back, whole, args):
            def run(heavy, light, *a):
                streams = (tuple([whole] * nch), heavy, light)
                outs = [sds(v.shape, bf) for v in a]
                stages = [sds((max(max(z), ALIGN), d), bf) for z in streams]
                return tuple(pl.pallas_call(
                    functools.partial(_exchange_kernel, nch, streams, back),
                    out_shape=outs + stages, in_specs=[ANY] * len(a), out_specs=[ANY] * (len(a) + 3),
                    scratch_shapes=[pltpu.SemaphoreType.DMA((3, nch, 3)), pltpu.SemaphoreType.DMA((3, nch, 3)),
                                    pltpu.SemaphoreType.DMA((3, 3)), pltpu.SemaphoreType.DMA((3, 3))],
                    compiler_params=pltpu.CompilerParams(collective_id=1 if back else 0, has_side_effects=True),
                    name='back' if back else 'there')(*a)[:len(a)])
            branches = [functools.partial(run, c, tuple([lo if n == len(cases) - 1 else 0] * nch))
                        for n, c in enumerate(cases)]
            out = lax.switch(case[0], branches, *args)
            return out[:nk], out[nk:2 * nk], out[2 * nk:]

        def ffn(base, roles, ranks, xin):
            nr = len(xin)
            xr = len(roles) * (4 * tok // ne) + 256
            n = tok // nch * len(roles) * len(ranks) // per
            return pl.pallas_call(
                functools.partial(_ffn_kernel, nch, base, roles, ranks),
                out_shape=[sds(a.shape, bf) for a in xin],
                in_specs=[SMEM] * 3 + [ANY] * (nr + 6), out_specs=[ANY] * nr,
                scratch_shapes=[pltpu.VMEM((2, xr, d), bf), pltpu.VMEM((2, d, f), bf), pltpu.VMEM((2, d, f), bf),
                                pltpu.VMEM((2, f, d), bf), pltpu.VMEM((256, f), bf),
                                pltpu.SemaphoreType.DMA((2, 3)), pltpu.SemaphoreType.DMA((2,)),
                                pltpu.SemaphoreType.DMA((2,))],
                compiler_params=params, name='ffn_' + '_'.join(map(str, roles + ranks)),
                cost_estimate=pl.CostEstimate(flops=6 * n * d * f, bytes_accessed=per * 3 * d * f * 2, transcendentals=0),
            )(cnt, perm, me, *xin, w1, w3, w2, *wp)

        far = tuple(range(1, nch))
        light, heavy = tuple(range(per // 2)), tuple(range(per // 2, per))

        def pairs(a, b):
            return [v for p in zip(a, b) for v in p]

        xlb, xho, xlo = exchange(False, lb, [*slb, *sho, *slo])
        held = lax.optimization_barrier((*shb, *xlb))
        shb, xlb = held[:nk], held[nk:]
        xhb = [shift(shb[k], k + 1) for k in range(nk)]
        yownl, *yl = ffn(lb, (0,) + far, light, [ownl, *pairs(xlb, xlo)])
        ylb, ylo = yl[::2], yl[1::2]
        zlb = [shift(ylb[k], nch - 1 - k) for k in range(nk)]
        ownh, yownl = lax.optimization_barrier((ownh, yownl))
        yownh, = ffn(hb, (0,), heavy, [ownh])
        held = lax.optimization_barrier((yownh, *xhb))
        yownh, xhb = held[0], held[1:]
        yh = ffn(hb, far, heavy, pairs(xhb, xho))
        yhb, yho = yh[::2], yh[1::2]
        zhb, zho, zlo = exchange(True, hb, [*yhb, *yho, *ylo])

        return pl.pallas_call(
            functools.partial(_unpack_kernel, nch, bases),
            out_shape=sds((tok, d), bf),
            in_specs=[SMEM] * 4 + [ANY] * (2 + 4 * nk), out_specs=ANY,
            scratch_shapes=[pltpu.VMEM((rows, d), bf), pltpu.VMEM((rows * nl, 128), jnp.float32),
                            pltpu.VMEM((tok * nl, 128), jnp.float32), pltpu.VMEM((tok, d), bf),
                            pltpu.SemaphoreType.DMA((nch,)), pltpu.SemaphoreType.DMA((CHUNKS,))],
            compiler_params=params, name='unpack',
        )(cnt, me, pos, wt, yownl, yownh, *[v for p in zip(zlb, zlo, zhb, zho) for v in p])

    return jax.shard_map(local, mesh=mesh, in_specs=(tok_spec,) * 5 + (w_spec,) * 3,
                         out_specs=tok_spec, check_vma=False)
```

```python
import functools

import jax
import jax.numpy as jnp
from jax import lax
from jax.experimental import pallas as pl
from jax.experimental.pallas import tpu as pltpu
from jax.sharding import PartitionSpec as P


ANY = pl.BlockSpec(memory_space=pltpu.HBM)
SMEM = pl.BlockSpec(memory_space=pltpu.SMEM)
VMEM = pl.BlockSpec(memory_space=pltpu.VMEM)
MESH = pl.DeviceIdType.MESH
ALIGN = 16
BIG = 64
VLIM = 66 * 10**6
CORES = 2
WCUT = 4


def _al(c):
    return (c + (ALIGN - 1)) // ALIGN * ALIGN


def _rows(op, src, s0, dst, d0, n, sem):
    def go(size, base):
        def body(i, _):
            s = pl.multiple_of(s0 + base + i * size, ALIGN)
            d = pl.multiple_of(d0 + base + i * size, ALIGN)
            cp = pltpu.make_async_copy(src.at[pl.ds(s, size)], dst.at[pl.ds(d, size)], sem)
            cp.start() if op == 0 else cp.wait()
            return 0
        return body
    nb = n // BIG
    lax.fori_loop(0, nb, go(BIG, 0), 0)
    lax.fori_loop(0, (n - nb * BIG) // ALIGN, go(ALIGN, nb * BIG), 0)


def _plan_kernel(nch, bases, cases, cnt, me, cntp, perm, first, case):
    g = nch * CORES
    ne = cnt.shape[0] // g
    per = ne // nch
    half = per // 2
    lb, hb = bases
    mine = (me[0] * CORES + me[1]) * ne
    level, light, at = [], 0, 0
    for j in range(nch):
        tot = [functools.reduce(lambda u, v: u + v, [cnt[s * ne + j * per + q] for s in range(g)]) for q in range(per)]
        rank = []
        for q in range(per):
            r = 0
            for p in range(per):
                if p != q:
                    r = r + ((tot[p] <= tot[q]) if p < q else (tot[p] < tot[q])).astype(jnp.int32)
            rank.append(r)
        order = []
        for r in range(per):
            o = 0
            for q in range(per):
                o = jnp.where(rank[q] == r, q, o)
            order.append(o)
            perm[j * per + r] = o
        sums = [0, 0]
        for s in range(g):
            al = []
            for r in range(per):
                c = cnt[s * ne + j * per + order[r]]
                cntp[s * ne + j * per + r] = c
                al.append(_al(c))
            for i in range(2):
                sums[i] = jnp.maximum(sums[i], functools.reduce(lambda u, v: u + v, al[i * half:(i + 1) * half]))
        light = jnp.maximum(light, sums[0])
        level.append(sums[1])
        for r in range(per):
            first[j * per + order[r]] = at
            at = at + _al(cnt[mine + j * per + order[r]])
    pick = len(cases) - 1
    for n, c in reversed(list(enumerate(cases[:-1]))):
        fits = functools.reduce(jnp.logical_and, [level[j] <= hb + c[j] for j in range(nch)] + [light <= lb])
        pick = jnp.where(fits, n, pick)
    case[0] = pick


def _parts(row, cntp, j, per):
    al = [_al(cntp[row + j * per + r]) for r in range(per)]
    half = per // 2
    return sum(al[:half]), sum(al[half:])


def _pieces(bases, tl, th):
    l1, h1 = jnp.minimum(tl, bases[0]), jnp.minimum(th, bases[1])
    return [(0, 0, l1), (1, l1, tl - l1), (2, tl, h1), (3, tl + h1, th - h1)]


def _widen(src, dst, lo, hi):
    nl = src.shape[1] // 128

    def body(b, _):
        v = src[pl.ds(pl.multiple_of(b * 16, 16), 16), :].astype(jnp.float32)
        for h in range(2):
            for c in range(nl):
                dst[pl.ds(pl.multiple_of((b * 2 + h) * 8 * nl + c * 8, 8), 8), :] = \
                    v[h * 8:h * 8 + 8, c * 128:c * 128 + 128]
        return 0
    lax.fori_loop(lo, hi, body, 0)


def _narrow(src, dst, lo, hi):
    nl = dst.shape[1] // 128

    def body(b, _):
        halves = []
        for h in range(2):
            halves.append(jnp.concatenate(
                [src[pl.ds(pl.multiple_of((b * 2 + h) * 8 * nl + c * 8, 8), 8), :] for c in range(nl)], axis=1))
        dst[pl.ds(pl.multiple_of(b * 16, 16), 16), :] = jnp.concatenate(halves, axis=0).astype(jnp.bfloat16)
        return 0
    lax.fori_loop(lo, hi, body, 0)


CHUNKS = 8


def _pack_kernel(nch, bases, cnt, me, pos, x, *refs):
    outs = refs[:2 + 4 * (nch - 1)]
    xv, xs, os_, ob, sem, xsem = refs[2 + 4 * (nch - 1):]
    tok, d = x.shape
    nl = d // 128
    ne = cnt.shape[0] // (nch * CORES)
    per = ne // nch
    chip = me[0]
    row = (chip * CORES + me[1]) * ne
    step = tok // CHUNKS

    def fetch(c):
        return pltpu.make_async_copy(x.at[pl.ds(c * step, step)], xv.at[pl.ds(c * step, step)], xsem.at[c])
    for c in range(CHUNKS):
        fetch(c).start()

    def move(g, _):
        for u in range(16):
            src = g * (16 * nl) + (u // 8) * (8 * nl) + u % 8
            os_[pl.ds(pos[g * 16 + u], nl, stride=8), :] = xs[pl.ds(src, nl, stride=8), :]
        return 0
    for c in range(CHUNKS):
        fetch(c).wait()
        _widen(xv, xs, c * step // 16, (c + 1) * step // 16)
    lax.fori_loop(0, tok // 16, move, 0)

    for op in (0, 1):
        start = 0
        for j in range(nch):
            tl, th = _parts(row, cnt, j, per)
            k = (j - chip + nch) % nch
            if op == 0:
                _narrow(os_, ob, start // 16, (start + tl + th) // 16)

            @pl.when(k == 0)
            def _(start=start, tl=tl, th=th):
                _rows(op, ob, start, outs[0], 0, tl, sem)
                _rows(op, ob, start + tl, outs[1], 0, th, sem)
            for kk in range(1, nch):
                @pl.when(k == kk)
                def _(start=start, tl=tl, th=th, kk=kk):
                    for i, at, n in _pieces(bases, tl, th):
                        _rows(op, ob, start + at, outs[2 + 4 * (kk - 1) + i], 0, n, sem)
            start = start + tl + th


def _ffn_kernel(nch, base, roles, ranks, cnt, perm, me, *refs):
    nr = sum(1 if k == 0 else 2 for k, _ in roles)
    xin, refs = refs[:nr], refs[nr:]
    (wa1, wa3, wa2, wb1, wb3, wb2), refs = refs[:6], refs[6:]
    yout, refs = refs[:nr], refs[nr:]
    xb, v1, v3, v2, hs, wsem, xsem, ysem = refs
    el, d, f = wa1.shape
    per = CORES * el
    ne = nch * per
    chip, core = me[0], me[1]
    place = []
    at = 0
    for k, _ in roles:
        place.append(at)
        at += 1 if k == 0 else 2

    def seg(q, role):
        k, held = role
        dev = ((chip - k + nch) % nch) * CORES + core
        first = dev * ne + chip * per
        off = 0
        for p in held:
            off = off + jnp.where(p < q, _al(cnt[first + p]), 0)
        n = _al(cnt[first + q])
        if held != ranks:
            n = jnp.where(jnp.logical_and(q >= held[0], q <= held[-1]), n, 0)
        return off, n

    def total(q):
        return sum(seg(q, role)[1] for role in roles)

    def rows(op, q, out):
        slot = lax.rem(q, 2)
        buf = xb.at[slot]
        at = 0
        for role, p in zip(roles, place):
            off, n = seg(q, role)
            n1 = n if role[0] == 0 else jnp.clip(base - off, 0, n)
            pieces = [(p, off, at, n1)]
            if role[0] != 0:
                pieces.append((p + 1, jnp.maximum(off - base, 0), at + n1, n - n1))
            for r, there, here, m in pieces:
                if out:
                    _rows(op, buf, here, yout[r], there, m, ysem.at[slot])
                else:
                    _rows(op, xin[r], there, buf, here, m, xsem.at[slot])
            at = at + n

    def weights(op, q):
        slot = lax.rem(q, 2)
        e = perm[chip * per + q]
        mine = lax.div(e, el) == core
        i = lax.rem(e, el)

        def go(srcs):
            for n, (s, v) in enumerate(zip(srcs, (v1, v3, v2))):
                m = v.shape[1] // WCUT
                for c in range(WCUT):
                    cp = pltpu.make_async_copy(s.at[i, pl.ds(c * m, m)], v.at[slot, pl.ds(c * m, m)], wsem.at[slot, n])
                    cp.start() if op == 0 else cp.wait()
        if op == 1:
            go((wa1, wa3, wa2))
        else:
            pl.when(mine)(lambda: go((wa1, wa3, wa2)))
            pl.when(jnp.logical_not(mine))(lambda: go((wb1, wb3, wb2)))

    def tile(slot, r0, tm):
        r0 = pl.multiple_of(r0, 128)
        fc = min(512, f)
        xt = xb[slot, pl.ds(r0, tm), :]
        for j in range(f // fc):
            a = jnp.dot(xt, v1[slot, :, j * fc:(j + 1) * fc], preferred_element_type=jnp.float32)
            b = jnp.dot(xt, v3[slot, :, j * fc:(j + 1) * fc], preferred_element_type=jnp.float32)
            hs[:tm, j * fc:(j + 1) * fc] = (jax.nn.silu(a) * b).astype(jnp.bfloat16)
        y = jnp.dot(hs[:tm, :], v2[slot], preferred_element_type=jnp.float32)
        xb[slot, pl.ds(r0, tm), :] = y.astype(jnp.bfloat16)

    weights(0, ranks[0])
    rows(0, ranks[0], False)

    def expert(q, _):
        slot = lax.rem(q, 2)

        @pl.when(q >= ranks[0] + 1)
        def _():
            rows(1, q - 1, True)

        @pl.when(q + 1 <= ranks[-1])
        def _():
            weights(0, q + 1)
            rows(0, q + 1, False)
        weights(1, q)
        rows(1, q, False)
        n = total(q)
        nbig = n // 256

        def big(t, _):
            tile(slot, t * 256, 256)
            return 0
        rest = n - nbig * 256
        nbig = nbig + (rest > 128).astype(jnp.int32)
        lax.fori_loop(0, nbig, big, 0)

        @pl.when(jnp.logical_and(rest > 0, rest <= 128))
        def _():
            tile(slot, nbig * 256, 128)
        rows(0, q, True)
        return 0
    lax.fori_loop(ranks[0], ranks[-1] + 1, expert, 0)
    rows(1, jnp.int32(ranks[-1]), True)


def _unpack_kernel(nch, bases, cnt, me, pos, w, *refs):
    ins = refs[:2 + 4 * (nch - 1)]
    out, zin, os_, xs, ov, sem, osem = refs[2 + 4 * (nch - 1):]
    tok, d = out.shape
    nl = d // 128
    ne = cnt.shape[0] // (nch * CORES)
    per = ne // nch
    chip = me[0]
    row = (chip * CORES + me[1]) * ne
    for op in (0, 1):
        start = 0
        for j in range(nch):
            tl, th = _parts(row, cnt, j, per)
            k = (j - chip + nch) % nch

            @pl.when(k == 0)
            def _(start=start, tl=tl, th=th, j=j):
                _rows(op, ins[0], 0, zin, start, tl, sem.at[j])
                _rows(op, ins[1], 0, zin, start + tl, th, sem.at[j])
            for kk in range(1, nch):
                @pl.when(k == kk)
                def _(start=start, tl=tl, th=th, kk=kk, j=j):
                    for i, at, n in _pieces(bases, tl, th):
                        _rows(op, ins[2 + 4 * (kk - 1) + i], 0, zin, start + at, n, sem.at[j])
            if op == 1:
                _widen(zin, os_, start // 16, (start + tl + th) // 16)
            start = start + tl + th

    def move(g, _):
        for u in range(16):
            dst = g * (16 * nl) + (u // 8) * (8 * nl) + u % 8
            xs[pl.ds(dst, nl, stride=8), :] = os_[pl.ds(pos[g * 16 + u], nl, stride=8), :] * w[g * 16 + u]
        return 0
    step = tok // CHUNKS

    def put(c):
        return pltpu.make_async_copy(ov.at[pl.ds(c * step, step)], out.at[pl.ds(c * step, step)], osem.at[c])
    for c in range(CHUNKS):
        lo, hi = c * step // 16, (c + 1) * step // 16
        lax.fori_loop(lo, hi, move, 0)
        _narrow(xs, ov, lo, hi)
        put(c).start()
    for c in range(CHUNKS):
        put(c).wait()


def _nothing_kernel(*refs):
    pass


def _cut(n, parts=3):
    u = n // ALIGN
    ends = [u * (i + 1) // parts * ALIGN for i in range(parts)]
    return [(lo, hi - lo) for lo, hi in zip([0] + ends[:-1], ends) if hi > lo]


def _exchange_kernel(nch, streams, back, *refs):
    ns, nk = len(streams), nch - 1
    src = [refs[i * nk:(i + 1) * nk] for i in range(ns)]
    dst = [refs[(ns + i) * nk:(ns + i + 1) * nk] for i in range(ns)]
    stage = refs[2 * ns * nk:2 * ns * nk + ns]
    send, recv, staged, passed = refs[2 * ns * nk + ns:]
    ep = lax.axis_index('ep')
    chip, core = lax.div(ep, CORES), lax.rem(ep, CORES)
    barrier = pltpu.get_barrier_semaphore()
    for k in range(1, nch):
        pl.semaphore_signal(barrier, inc=1, device_id={'ep': lax.rem(chip + k, nch) * CORES + core}, device_id_type=MESH)
    pl.semaphore_wait(barrier, nch - 1)
    opp = nch // 2
    turn = 1 - 2 * core

    def ring(c):
        return lax.rem(c + nch, nch)

    def copy(s, d, cut, a, b, to):
        return pltpu.make_async_remote_copy(
            src_ref=s.at[pl.ds(*cut)], dst_ref=d.at[pl.ds(*cut)], send_sem=a, recv_sem=b,
            device_id={'ep': to * CORES + core}, device_id_type=MESH)

    def each(what):
        for i, sizes in enumerate(streams):
            n = max(sizes)
            if not n:
                continue

            def guard(s, o, i=i, sizes=sizes):
                c = s if back else o
                if all(sizes):
                    return lambda f: f()
                return pl.when(functools.reduce(jnp.logical_or, [c == j for j in range(nch) if sizes[j]]))
            what(i, n, guard)

    def first_hop(i, p, cut):
        return copy(src[i][opp - 1], stage[i], cut, send.at[i, opp, p], staged.at[i, p], ring(chip + turn))

    def second_hop(i, p, cut):
        return copy(stage[i], dst[i][opp - 1], cut, passed.at[i, p], recv.at[i, opp, p], ring(chip + turn))

    def near(i, k, n):
        return copy(src[i][k - 1], dst[i][k - 1], (0, n), send.at[i, k, 0], recv.at[i, k, 0],
                    ring(chip - k if back else chip + k))

    def start(i, n, guard):
        @guard(chip, ring(chip + opp))
        def _():
            for p, cut in enumerate(_cut(n)):
                first_hop(i, p, cut).start()
        for k in range(1, nch):
            if k != opp:
                @guard(chip, ring(chip + k))
                def _(k=k):
                    near(i, k, n).start()

    def relay(i, n, guard):
        @guard(ring(chip - turn), ring(chip + turn))
        def _():
            for p, cut in enumerate(_cut(n)):
                first_hop(i, p, cut).wait_recv()
                second_hop(i, p, cut).start()

    def finish(i, n, guard):
        @guard(chip, ring(chip + opp))
        def _():
            for p, cut in enumerate(_cut(n)):
                first_hop(i, p, cut).wait_send()

        @guard(ring(chip - turn), ring(chip + turn))
        def _():
            for p, cut in enumerate(_cut(n)):
                second_hop(i, p, cut).wait_send()

        @guard(ring(chip + opp), chip)
        def _():
            for p, cut in enumerate(_cut(n)):
                second_hop(i, p, cut).wait_recv()
        for k in range(1, nch):
            if k != opp:
                @guard(chip, ring(chip + k))
                def _(k=k):
                    near(i, k, n).wait_send()

                @guard(ring(chip + k if back else chip - k), chip)
                def _(k=k):
                    near(i, k, n).wait_recv()
    each(start)
    each(relay)
    each(finish)


def _cases(nch, steps, full):
    cases = [tuple([0] * nch)]
    for s in steps:
        for j in range(nch):
            cases.append(tuple(s if i == j else 0 for i in range(nch)))
    for j in range(nch):
        for l in range(j + 1, nch):
            for s in steps[:2]:
                cases.append(tuple(s if i in (j, l) else 0 for i in range(nch)))
    for s in steps[1::2]:
        cases.append(tuple([s] * nch))
    cases.append(tuple([full] * nch))
    return cases


def solution(mesh):
    g_ = mesh.shape['ep']
    tok_spec = P(('dp', 'ep'), None)
    w_spec = P('ep', None, None)
    nch = g_ // CORES

    def local(x, idx, w, slot, counts, w1, w3, w2):
        tok, d = x.shape
        el, _, f = w1.shape
        per = CORES * el
        ne = g_ * el
        nl = d // 128
        half = per // 2 * (4 * tok // ne)
        bases = (_al(tok * 17 // 128), _al(tok * 17 // 128))
        lb, hb = bases
        steps = tuple(_al(tok * v // 128) for v in (13, 15, 26, 28))
        lo, ho = half - lb, half - hb
        cases = _cases(nch, steps, ho)
        bf, i32 = jnp.bfloat16, jnp.int32
        nk = nch - 1
        ep = lax.axis_index('ep')
        me = jnp.stack([ep // CORES, ep % CORES]).astype(i32)
        sds = jax.ShapeDtypeStruct
        params = pltpu.CompilerParams(vmem_limit_bytes=VLIM)

        gathered = lax.all_gather(counts[0], 'ep').reshape(-1)
        cnt, perm, first, case = pl.pallas_call(
            functools.partial(_plan_kernel, nch, bases, tuple(cases)),
            out_shape=[sds((g_ * ne,), i32), sds((ne,), i32), sds((ne,), i32), sds((1,), i32)],
            in_specs=[SMEM] * 2, out_specs=[SMEM] * 4, name='plan')(gathered, me)

        first, *wx = lax.optimization_barrier((first, w1, w3, w2))
        swap = [(2 * s + c, 2 * s + 1 - c) for s in range(nch) for c in range(CORES)]
        wp = [lax.ppermute(a, 'ep', swap) for a in wx]

        e = idx.reshape(tok)
        row = slot.reshape(tok) + jnp.sum(
            jnp.where(e[None, :] == jnp.arange(ne)[:, None], first[:, None], 0), axis=0)
        pos = (row // 8) * (8 * nl) + row % 8
        wt = w.reshape(tok)

        rows = tok + ALIGN * ne
        packed = pl.pallas_call(
            functools.partial(_pack_kernel, nch, bases),
            out_shape=[sds((half, d), bf)] * 2 + [sds((n, d), bf) for n in (lb, lo, hb, ho)] * nk,
            in_specs=[SMEM, SMEM, SMEM, ANY], out_specs=[ANY] * (2 + 4 * nk),
            scratch_shapes=[pltpu.VMEM((tok, d), bf), pltpu.VMEM((tok * nl, 128), jnp.float32),
                            pltpu.VMEM((rows * nl, 128), jnp.float32), pltpu.VMEM((rows, d), bf),
                            pltpu.SemaphoreType.DMA, pltpu.SemaphoreType.DMA((CHUNKS,))],
            compiler_params=params, name='pack',
            cost_estimate=pl.CostEstimate(flops=2 * 10**9, bytes_accessed=3 * tok * d * 2, transcendentals=0),
        )(cnt, me, pos, x)
        ownl, ownh = packed[:2]
        slb, slo, shb, sho = [[packed[2 + 4 * k + i] for k in range(nk)] for i in range(4)]

        def shift(a, k):
            return lax.ppermute(a, 'ep', [(CORES * s + c, CORES * ((s + k) % nch) + c)
                                          for s in range(nch) for c in range(CORES)])

        def move(streams, back, ident, *a):
            ns = len(streams)
            outs = [sds(v.shape, bf) for v in a]
            if not any(map(any, streams)):
                return tuple(pl.pallas_call(_nothing_kernel, out_shape=outs, in_specs=[ANY] * len(a),
                                            out_specs=[ANY] * len(a), name='nothing')(*a))
            stages = [sds((max(max(z), ALIGN), d), bf) for z in streams]
            return tuple(pl.pallas_call(
                functools.partial(_exchange_kernel, nch, streams, back),
                out_shape=outs + stages, in_specs=[ANY] * len(a), out_specs=[ANY] * (len(a) + ns),
                scratch_shapes=[pltpu.SemaphoreType.DMA((ns, nch, 3)), pltpu.SemaphoreType.DMA((ns, nch, 3)),
                                pltpu.SemaphoreType.DMA((ns, 3)), pltpu.SemaphoreType.DMA((ns, 3))],
                compiler_params=pltpu.CompilerParams(collective_id=ident, has_side_effects=True),
                name='back' if back else 'there')(*a)[:len(a)])

        def choose(make, back, ident, args):
            branches = [functools.partial(move, make(n, c), back, ident) for n, c in enumerate(cases)]
            out = lax.switch(case[0], branches, *args)
            return [out[i * nk:(i + 1) * nk] for i in range(len(args) // nk)]

        def lights(n):
            return (lo if n == len(cases) - 1 else 0,) * nch

        def ffn(name, base, roles, ranks, xin):
            nr = len(xin)
            xr = len(roles) * (4 * tok // ne) + 256
            n = sum(tok // nch * len(held) // per for _, held in roles)
            return pl.pallas_call(
                functools.partial(_ffn_kernel, nch, base, roles, ranks),
                out_shape=[sds(a.shape, bf) for a in xin],
                in_specs=[SMEM] * 3 + [ANY] * (nr + 6), out_specs=[ANY] * nr,
                scratch_shapes=[pltpu.VMEM((2, xr, d), bf), pltpu.VMEM((2, d, f), bf), pltpu.VMEM((2, d, f), bf),
                                pltpu.VMEM((2, f, d), bf), pltpu.VMEM((256, f), bf),
                                pltpu.SemaphoreType.DMA((2, 3)), pltpu.SemaphoreType.DMA((2,)),
                                pltpu.SemaphoreType.DMA((2,))],
                compiler_params=params, name=name,
                cost_estimate=pl.CostEstimate(flops=6 * n * d * f, bytes_accessed=per * 3 * d * f * 2, transcendentals=0),
            )(cnt, perm, me, *xin, w1, w3, w2, *wp)

        light, heavy = tuple(range(per // 2)), tuple(range(per // 2, per))

        def pairs(a, b):
            return [v for p in zip(a, b) for v in p]

        def far(held):
            return tuple((k, held) for k in range(1, nch))

        xlb = [shift(slb[k], k + 1) for k in range(nk)]
        held = lax.optimization_barrier((*shb, *slb))
        xhb = [shift(held[k], k + 1) for k in range(nk)]
        xlo = lax.cond(case[0] == len(cases) - 1, functools.partial(move, ((lo,) * nch,), False, 2),
                       functools.partial(move, ((0,) * nch,), False, 2), *slo)
        yownl, yownh = ffn('own', hb, ((0, light), (0, heavy)), light + heavy, [ownl, ownh])
        held = lax.optimization_barrier((yownl, *xlb))
        yownl, xlb = held[0], held[1:]
        yl = ffn('light', lb, far(light), light, pairs(xlb, xlo))
        ylb, ylo = yl[::2], yl[1::2]
        held = lax.optimization_barrier((*sho, *ylb))
        xho, = choose(lambda n, c: (c,), False, 0, held[:nk])
        held = lax.optimization_barrier((*ylb, *xho))
        ylb, xho = held[:nk], held[nk:]
        zlb = [shift(ylb[k], nch - 1 - k) for k in range(nk)]
        yh = ffn('heavy', hb, far(heavy), heavy, pairs(xhb, xho))
        yhb, yho = yh[::2], yh[1::2]
        zhb, zho, zlo = choose(lambda n, c: ((hb,) * nch, c, lights(n)), True, 1, [*yhb, *yho, *ylo])

        return pl.pallas_call(
            functools.partial(_unpack_kernel, nch, bases),
            out_shape=sds((tok, d), bf),
            in_specs=[SMEM] * 4 + [ANY] * (2 + 4 * nk), out_specs=ANY,
            scratch_shapes=[pltpu.VMEM((rows, d), bf), pltpu.VMEM((rows * nl, 128), jnp.float32),
                            pltpu.VMEM((tok * nl, 128), jnp.float32), pltpu.VMEM((tok, d), bf),
                            pltpu.SemaphoreType.DMA((nch,)), pltpu.SemaphoreType.DMA((CHUNKS,))],
            compiler_params=params, name='unpack',
        )(cnt, me, pos, wt, yownl, yownh, *[v for p in zip(zlb, zlo, zhb, zho) for v in p])

    return jax.shard_map(local, mesh=mesh, in_specs=(tok_spec,) * 5 + (w_spec,) * 3,
                         out_specs=tok_spec, check_vma=False)
```

```python
import functools

import jax
import jax.numpy as jnp
from jax import lax
from jax.experimental import pallas as pl
from jax.experimental.pallas import tpu as pltpu
from jax.sharding import PartitionSpec as P


ANY = pl.BlockSpec(memory_space=pltpu.HBM)
SMEM = pl.BlockSpec(memory_space=pltpu.SMEM)
VMEM = pl.BlockSpec(memory_space=pltpu.VMEM)
MESH = pl.DeviceIdType.MESH
ALIGN = 16
BIG = 64
VLIM = 66 * 10**6
CORES = 2
WCUT = 4


def _al(c):
    return (c + (ALIGN - 1)) // ALIGN * ALIGN


def _rows(op, src, s0, dst, d0, n, sem):
    def go(size, base):
        def body(i, _):
            s = pl.multiple_of(s0 + base + i * size, ALIGN)
            d = pl.multiple_of(d0 + base + i * size, ALIGN)
            cp = pltpu.make_async_copy(src.at[pl.ds(s, size)], dst.at[pl.ds(d, size)], sem)
            cp.start() if op == 0 else cp.wait()
            return 0
        return body
    nb = n // BIG
    lax.fori_loop(0, nb, go(BIG, 0), 0)
    lax.fori_loop(0, (n - nb * BIG) // ALIGN, go(ALIGN, nb * BIG), 0)


def _plan_kernel(nch, bases, cases, cnt, me, cntp, perm, first, case):
    g = nch * CORES
    ne = cnt.shape[0] // g
    per = ne // nch
    half = per // 2
    lb, hb = bases
    mine = (me[0] * CORES + me[1]) * ne
    level, light, at = [], 0, 0
    for j in range(nch):
        tot = [functools.reduce(lambda u, v: u + v, [cnt[s * ne + j * per + q] for s in range(g)]) for q in range(per)]
        rank = []
        for q in range(per):
            r = 0
            for p in range(per):
                if p != q:
                    r = r + ((tot[p] <= tot[q]) if p < q else (tot[p] < tot[q])).astype(jnp.int32)
            rank.append(r)
        order = []
        for r in range(per):
            o = 0
            for q in range(per):
                o = jnp.where(rank[q] == r, q, o)
            order.append(o)
            perm[j * per + r] = o
        sums = [0, 0]
        for s in range(g):
            al = []
            for r in range(per):
                c = cnt[s * ne + j * per + order[r]]
                cntp[s * ne + j * per + r] = c
                al.append(_al(c))
            for i in range(2):
                sums[i] = jnp.maximum(sums[i], functools.reduce(lambda u, v: u + v, al[i * half:(i + 1) * half]))
        light = jnp.maximum(light, sums[0])
        level.append(sums[1])
        for r in range(per):
            first[j * per + order[r]] = at
            at = at + _al(cnt[mine + j * per + order[r]])
    pick = len(cases) - 1
    for n, c in reversed(list(enumerate(cases[:-1]))):
        fits = functools.reduce(jnp.logical_and, [level[j] <= hb + c[j] for j in range(nch)] + [light <= lb])
        pick = jnp.where(fits, n, pick)
    case[0] = pick


def _parts(row, cntp, j, per):
    al = [_al(cntp[row + j * per + r]) for r in range(per)]
    half = per // 2
    return sum(al[:half]), sum(al[half:])


def _pieces(bases, tl, th):
    l1, h1 = jnp.minimum(tl, bases[0]), jnp.minimum(th, bases[1])
    return [(0, 0, l1), (1, l1, tl - l1), (2, tl, h1), (3, tl + h1, th - h1)]


def _widen(src, dst, lo, hi):
    nl = src.shape[1] // 128

    def body(b, _):
        v = src[pl.ds(pl.multiple_of(b * 16, 16), 16), :].astype(jnp.float32)
        for h in range(2):
            for c in range(nl):
                dst[pl.ds(pl.multiple_of((b * 2 + h) * 8 * nl + c * 8, 8), 8), :] = \
                    v[h * 8:h * 8 + 8, c * 128:c * 128 + 128]
        return 0
    lax.fori_loop(lo, hi, body, 0)


def _narrow(src, dst, lo, hi):
    nl = dst.shape[1] // 128

    def body(b, _):
        halves = []
        for h in range(2):
            halves.append(jnp.concatenate(
                [src[pl.ds(pl.multiple_of((b * 2 + h) * 8 * nl + c * 8, 8), 8), :] for c in range(nl)], axis=1))
        dst[pl.ds(pl.multiple_of(b * 16, 16), 16), :] = jnp.concatenate(halves, axis=0).astype(jnp.bfloat16)
        return 0
    lax.fori_loop(lo, hi, body, 0)


CHUNKS = 8


def _pack_kernel(nch, bases, cnt, me, pos, x, *refs):
    outs = refs[:2 + 4 * (nch - 1)]
    xv, xs, os_, ob, sem, xsem = refs[2 + 4 * (nch - 1):]
    tok, d = x.shape
    nl = d // 128
    ne = cnt.shape[0] // (nch * CORES)
    per = ne // nch
    chip = me[0]
    row = (chip * CORES + me[1]) * ne
    step = tok // CHUNKS

    def fetch(c):
        return pltpu.make_async_copy(x.at[pl.ds(c * step, step)], xv.at[pl.ds(c * step, step)], xsem.at[c])
    for c in range(CHUNKS):
        fetch(c).start()

    def move(g, _):
        for u in range(16):
            src = g * (16 * nl) + (u // 8) * (8 * nl) + u % 8
            os_[pl.ds(pos[g * 16 + u], nl, stride=8), :] = xs[pl.ds(src, nl, stride=8), :]
        return 0
    for c in range(CHUNKS):
        fetch(c).wait()
        _widen(xv, xs, c * step // 16, (c + 1) * step // 16)
    lax.fori_loop(0, tok // 16, move, 0)

    for op in (0, 1):
        start = 0
        for j in range(nch):
            tl, th = _parts(row, cnt, j, per)
            k = (j - chip + nch) % nch
            if op == 0:
                _narrow(os_, ob, start // 16, (start + tl + th) // 16)

            @pl.when(k == 0)
            def _(start=start, tl=tl, th=th):
                _rows(op, ob, start, outs[0], 0, tl, sem)
                _rows(op, ob, start + tl, outs[1], 0, th, sem)
            for kk in range(1, nch):
                @pl.when(k == kk)
                def _(start=start, tl=tl, th=th, kk=kk):
                    for i, at, n in _pieces(bases, tl, th):
                        _rows(op, ob, start + at, outs[2 + 4 * (kk - 1) + i], 0, n, sem)
            start = start + tl + th


def _ffn_kernel(nch, base, roles, ranks, cnt, perm, me, *refs):
    nr = sum(1 if k == 0 else 2 for k, _ in roles)
    xin, refs = refs[:nr], refs[nr:]
    (wa1, wa3, wa2, wb1, wb3, wb2), refs = refs[:6], refs[6:]
    yout, refs = refs[:nr], refs[nr:]
    xb, v1, v3, v2, hs, wsem, xsem, ysem = refs
    el, d, f = wa1.shape
    per = CORES * el
    ne = nch * per
    chip, core = me[0], me[1]
    place = []
    at = 0
    for k, _ in roles:
        place.append(at)
        at += 1 if k == 0 else 2

    def seg(q, role):
        k, held = role
        dev = ((chip - k + nch) % nch) * CORES + core
        first = dev * ne + chip * per
        off = 0
        for p in held:
            off = off + jnp.where(p < q, _al(cnt[first + p]), 0)
        n = _al(cnt[first + q])
        if held != ranks:
            n = jnp.where(jnp.logical_and(q >= held[0], q <= held[-1]), n, 0)
        return off, n

    def total(q):
        return sum(seg(q, role)[1] for role in roles)

    def rows(op, q, out):
        slot = lax.rem(q, 2)
        buf = xb.at[slot]
        at = 0
        for role, p in zip(roles, place):
            off, n = seg(q, role)
            n1 = n if role[0] == 0 else jnp.clip(base - off, 0, n)
            pieces = [(p, off, at, n1)]
            if role[0] != 0:
                pieces.append((p + 1, jnp.maximum(off - base, 0), at + n1, n - n1))
            for r, there, here, m in pieces:
                if out:
                    _rows(op, buf, here, yout[r], there, m, ysem.at[slot])
                else:
                    _rows(op, xin[r], there, buf, here, m, xsem.at[slot])
            at = at + n

    def weights(op, q):
        slot = lax.rem(q, 2)
        e = perm[chip * per + q]
        mine = lax.div(e, el) == core
        i = lax.rem(e, el)

        def go(srcs):
            for n, (s, v) in enumerate(zip(srcs, (v1, v3, v2))):
                m = v.shape[1] // WCUT
                for c in range(WCUT):
                    cp = pltpu.make_async_copy(s.at[i, pl.ds(c * m, m)], v.at[slot, pl.ds(c * m, m)], wsem.at[slot, n])
                    cp.start() if op == 0 else cp.wait()
        if op == 1:
            go((wa1, wa3, wa2))
        else:
            pl.when(mine)(lambda: go((wa1, wa3, wa2)))
            pl.when(jnp.logical_not(mine))(lambda: go((wb1, wb3, wb2)))

    def tile(slot, r0, tm):
        r0 = pl.multiple_of(r0, 128)
        fc = min(512, f)
        xt = xb[slot, pl.ds(r0, tm), :]
        for j in range(f // fc):
            a = jnp.dot(xt, v1[slot, :, j * fc:(j + 1) * fc], preferred_element_type=jnp.float32)
            b = jnp.dot(xt, v3[slot, :, j * fc:(j + 1) * fc], preferred_element_type=jnp.float32)
            hs[:tm, j * fc:(j + 1) * fc] = (jax.nn.silu(a) * b).astype(jnp.bfloat16)
        y = jnp.dot(hs[:tm, :], v2[slot], preferred_element_type=jnp.float32)
        xb[slot, pl.ds(r0, tm), :] = y.astype(jnp.bfloat16)

    weights(0, ranks[0])
    rows(0, ranks[0], False)

    def expert(q, _):
        slot = lax.rem(q, 2)

        @pl.when(q >= ranks[0] + 1)
        def _():
            rows(1, q - 1, True)

        @pl.when(q + 1 <= ranks[-1])
        def _():
            weights(0, q + 1)
            rows(0, q + 1, False)
        weights(1, q)
        rows(1, q, False)
        n = total(q)
        nbig = n // 256

        def big(t, _):
            tile(slot, t * 256, 256)
            return 0
        rest = n - nbig * 256
        nbig = nbig + (rest > 128).astype(jnp.int32)
        lax.fori_loop(0, nbig, big, 0)

        @pl.when(jnp.logical_and(rest > 0, rest <= 128))
        def _():
            tile(slot, nbig * 256, 128)
        rows(0, q, True)
        return 0
    lax.fori_loop(ranks[0], ranks[-1] + 1, expert, 0)
    rows(1, jnp.int32(ranks[-1]), True)


def _unpack_kernel(nch, bases, cnt, me, pos, w, *refs):
    ins = refs[:2 + 4 * (nch - 1)]
    out, zin, os_, xs, ov, sem, osem = refs[2 + 4 * (nch - 1):]
    tok, d = out.shape
    nl = d // 128
    ne = cnt.shape[0] // (nch * CORES)
    per = ne // nch
    chip = me[0]
    row = (chip * CORES + me[1]) * ne
    for op in (0, 1):
        start = 0
        for j in range(nch):
            tl, th = _parts(row, cnt, j, per)
            k = (j - chip + nch) % nch

            @pl.when(k == 0)
            def _(start=start, tl=tl, th=th, j=j):
                _rows(op, ins[0], 0, zin, start, tl, sem.at[j])
                _rows(op, ins[1], 0, zin, start + tl, th, sem.at[j])
            for kk in range(1, nch):
                @pl.when(k == kk)
                def _(start=start, tl=tl, th=th, kk=kk, j=j):
                    for i, at, n in _pieces(bases, tl, th):
                        _rows(op, ins[2 + 4 * (kk - 1) + i], 0, zin, start + at, n, sem.at[j])
            if op == 1:
                _widen(zin, os_, start // 16, (start + tl + th) // 16)
            start = start + tl + th

    def move(g, _):
        for u in range(16):
            dst = g * (16 * nl) + (u // 8) * (8 * nl) + u % 8
            xs[pl.ds(dst, nl, stride=8), :] = os_[pl.ds(pos[g * 16 + u], nl, stride=8), :] * w[g * 16 + u]
        return 0
    step = tok // CHUNKS

    def put(c):
        return pltpu.make_async_copy(ov.at[pl.ds(c * step, step)], out.at[pl.ds(c * step, step)], osem.at[c])
    for c in range(CHUNKS):
        lo, hi = c * step // 16, (c + 1) * step // 16
        lax.fori_loop(lo, hi, move, 0)
        _narrow(xs, ov, lo, hi)
        put(c).start()
    for c in range(CHUNKS):
        put(c).wait()


def _nothing_kernel(*refs):
    pass


def _cut(n):
    parts = 3 if n > 512 else 2
    u = n // ALIGN
    ends = [u * (i + 1) // parts * ALIGN for i in range(parts)]
    return [(lo, hi - lo) for lo, hi in zip([0] + ends[:-1], ends) if hi > lo]


def _exchange_kernel(nch, streams, back, *refs):
    ns, nk = len(streams), nch - 1
    src = [refs[i * nk:(i + 1) * nk] for i in range(ns)]
    dst = [refs[(ns + i) * nk:(ns + i + 1) * nk] for i in range(ns)]
    stage = refs[2 * ns * nk:2 * ns * nk + ns]
    send, recv, staged, passed = refs[2 * ns * nk + ns:]
    ep = lax.axis_index('ep')
    chip, core = lax.div(ep, CORES), lax.rem(ep, CORES)
    barrier = pltpu.get_barrier_semaphore()
    for k in range(1, nch):
        pl.semaphore_signal(barrier, inc=1, device_id={'ep': lax.rem(chip + k, nch) * CORES + core}, device_id_type=MESH)
    pl.semaphore_wait(barrier, nch - 1)
    opp = nch // 2
    turn = 1 - 2 * core

    def ring(c):
        return lax.rem(c + nch, nch)

    def copy(s, d, cut, a, b, to):
        return pltpu.make_async_remote_copy(
            src_ref=s.at[pl.ds(*cut)], dst_ref=d.at[pl.ds(*cut)], send_sem=a, recv_sem=b,
            device_id={'ep': to * CORES + core}, device_id_type=MESH)

    def each(what):
        for i, sizes in enumerate(streams):
            n = max(sizes)
            if not n:
                continue

            def guard(s, o, i=i, sizes=sizes):
                c = s if back else o
                if all(sizes):
                    return lambda f: f()
                return pl.when(functools.reduce(jnp.logical_or, [c == j for j in range(nch) if sizes[j]]))
            what(i, n, guard)

    def first_hop(i, p, cut):
        return copy(src[i][opp - 1], stage[i], cut, send.at[i, opp, p], staged.at[i, p], ring(chip + turn))

    def second_hop(i, p, cut):
        return copy(stage[i], dst[i][opp - 1], cut, passed.at[i, p], recv.at[i, opp, p], ring(chip + turn))

    def near(i, k, n):
        return copy(src[i][k - 1], dst[i][k - 1], (0, n), send.at[i, k, 0], recv.at[i, k, 0],
                    ring(chip - k if back else chip + k))

    def start(i, n, guard):
        @guard(chip, ring(chip + opp))
        def _():
            for p, cut in enumerate(_cut(n)):
                first_hop(i, p, cut).start()
        for k in range(1, nch):
            if k != opp:
                @guard(chip, ring(chip + k))
                def _(k=k):
                    near(i, k, n).start()

    def relay(i, n, guard):
        @guard(ring(chip - turn), ring(chip + turn))
        def _():
            for p, cut in enumerate(_cut(n)):
                first_hop(i, p, cut).wait_recv()
                second_hop(i, p, cut).start()

    def finish(i, n, guard):
        @guard(chip, ring(chip + opp))
        def _():
            for p, cut in enumerate(_cut(n)):
                first_hop(i, p, cut).wait_send()

        @guard(ring(chip - turn), ring(chip + turn))
        def _():
            for p, cut in enumerate(_cut(n)):
                second_hop(i, p, cut).wait_send()

        @guard(ring(chip + opp), chip)
        def _():
            for p, cut in enumerate(_cut(n)):
                second_hop(i, p, cut).wait_recv()
        for k in range(1, nch):
            if k != opp:
                @guard(chip, ring(chip + k))
                def _(k=k):
                    near(i, k, n).wait_send()

                @guard(ring(chip + k if back else chip - k), chip)
                def _(k=k):
                    near(i, k, n).wait_recv()
    each(start)
    each(relay)
    each(finish)


def _cases(nch, steps, full):
    cases = [tuple([0] * nch)]
    for j in range(nch):
        for l in range(j + 1, nch):
            for s in steps[:2]:
                cases.append(tuple(s if i in (j, l) else 0 for i in range(nch)))
    for s in steps[2:]:
        for j in range(nch):
            cases.append(tuple(s if i == j else 0 for i in range(nch)))
    for s in steps[1::2]:
        cases.append(tuple([s] * nch))
    cases.append(tuple([full] * nch))
    return cases


def solution(mesh):
    g_ = mesh.shape['ep']
    tok_spec = P(('dp', 'ep'), None)
    w_spec = P('ep', None, None)
    nch = g_ // CORES

    def local(x, idx, w, slot, counts, w1, w3, w2):
        tok, d = x.shape
        el, _, f = w1.shape
        per = CORES * el
        ne = g_ * el
        nl = d // 128
        half = per // 2 * (4 * tok // ne)
        bases = (_al(tok * 33 // 256), _al(tok * 33 // 256))
        lb, hb = bases
        steps = tuple(_al(int(tok * v / 128)) for v in (13.5, 15.5, 26.5, 28.5))
        lo, ho = half - lb, half - hb
        cases = _cases(nch, steps, ho)
        bf, i32 = jnp.bfloat16, jnp.int32
        nk = nch - 1
        ep = lax.axis_index('ep')
        me = jnp.stack([ep // CORES, ep % CORES]).astype(i32)
        sds = jax.ShapeDtypeStruct
        params = pltpu.CompilerParams(vmem_limit_bytes=VLIM)

        gathered = lax.all_gather(counts[0], 'ep').reshape(-1)
        cnt, perm, first, case = pl.pallas_call(
            functools.partial(_plan_kernel, nch, bases, tuple(cases)),
            out_shape=[sds((g_ * ne,), i32), sds((ne,), i32), sds((ne,), i32), sds((1,), i32)],
            in_specs=[SMEM] * 2, out_specs=[SMEM] * 4, name='plan')(gathered, me)

        first, *wx = lax.optimization_barrier((first, w1, w3, w2))
        swap = [(2 * s + c, 2 * s + 1 - c) for s in range(nch) for c in range(CORES)]
        wp = [lax.ppermute(a, 'ep', swap) for a in wx]

        e = idx.reshape(tok)
        row = slot.reshape(tok) + jnp.sum(
            jnp.where(e[None, :] == jnp.arange(ne)[:, None], first[:, None], 0), axis=0)
        pos = (row // 8) * (8 * nl) + row % 8
        wt = w.reshape(tok)

        rows = tok + ALIGN * ne
        packed = pl.pallas_call(
            functools.partial(_pack_kernel, nch, bases),
            out_shape=[sds((half, d), bf)] * 2 + [sds((n, d), bf) for n in (lb, lo, hb, ho)] * nk,
            in_specs=[SMEM, SMEM, SMEM, ANY], out_specs=[ANY] * (2 + 4 * nk),
            scratch_shapes=[pltpu.VMEM((tok, d), bf), pltpu.VMEM((tok * nl, 128), jnp.float32),
                            pltpu.VMEM((rows * nl, 128), jnp.float32), pltpu.VMEM((rows, d), bf),
                            pltpu.SemaphoreType.DMA, pltpu.SemaphoreType.DMA((CHUNKS,))],
            compiler_params=params, name='pack',
            cost_estimate=pl.CostEstimate(flops=2 * 10**9, bytes_accessed=3 * tok * d * 2, transcendentals=0),
        )(cnt, me, pos, x)
        ownl, ownh = packed[:2]
        slb, slo, shb, sho = [[packed[2 + 4 * k + i] for k in range(nk)] for i in range(4)]

        def shift(a, k):
            return lax.ppermute(a, 'ep', [(CORES * s + c, CORES * ((s + k) % nch) + c)
                                          for s in range(nch) for c in range(CORES)])

        def move(streams, back, ident, *a):
            ns = len(streams)
            outs = [sds(v.shape, bf) for v in a]
            if not any(map(any, streams)):
                return tuple(pl.pallas_call(_nothing_kernel, out_shape=outs, in_specs=[ANY] * len(a),
                                            out_specs=[ANY] * len(a), name='nothing')(*a))
            stages = [sds((max(max(z), ALIGN), d), bf) for z in streams]
            return tuple(pl.pallas_call(
                functools.partial(_exchange_kernel, nch, streams, back),
                out_shape=outs + stages, in_specs=[ANY] * len(a), out_specs=[ANY] * (len(a) + ns),
                scratch_shapes=[pltpu.SemaphoreType.DMA((ns, nch, 3)), pltpu.SemaphoreType.DMA((ns, nch, 3)),
                                pltpu.SemaphoreType.DMA((ns, 3)), pltpu.SemaphoreType.DMA((ns, 3))],
                compiler_params=pltpu.CompilerParams(collective_id=ident, has_side_effects=True),
                name='back' if back else 'there')(*a)[:len(a)])

        def choose(make, back, ident, args):
            branches = [functools.partial(move, make(n, c), back, ident) for n, c in enumerate(cases)]
            out = lax.switch(case[0], branches, *args)
            return [out[i * nk:(i + 1) * nk] for i in range(len(args) // nk)]

        def lights(n):
            return (lo if n == len(cases) - 1 else 0,) * nch

        def ffn(name, base, roles, ranks, xin):
            nr = len(xin)
            xr = len(roles) * (4 * tok // ne) + 256
            n = sum(tok // nch * len(held) // per for _, held in roles)
            return pl.pallas_call(
                functools.partial(_ffn_kernel, nch, base, roles, ranks),
                out_shape=[sds(a.shape, bf) for a in xin],
                in_specs=[SMEM] * 3 + [ANY] * (nr + 6), out_specs=[ANY] * nr,
                scratch_shapes=[pltpu.VMEM((2, xr, d), bf), pltpu.VMEM((2, d, f), bf), pltpu.VMEM((2, d, f), bf),
                                pltpu.VMEM((2, f, d), bf), pltpu.VMEM((256, f), bf),
                                pltpu.SemaphoreType.DMA((2, 3)), pltpu.SemaphoreType.DMA((2,)),
                                pltpu.SemaphoreType.DMA((2,))],
                compiler_params=params, name=name,
                cost_estimate=pl.CostEstimate(flops=6 * n * d * f, bytes_accessed=per * 3 * d * f * 2, transcendentals=0),
            )(cnt, perm, me, *xin, w1, w3, w2, *wp)

        light, heavy = tuple(range(per // 2)), tuple(range(per // 2, per))

        def pairs(a, b):
            return [v for p in zip(a, b) for v in p]

        def far(held):
            return tuple((k, held) for k in range(1, nch))

        xlb = [shift(slb[k], k + 1) for k in range(nk)]
        held = lax.optimization_barrier((*shb, *slb))
        xhb = [shift(held[k], k + 1) for k in range(nk)]
        xlo = lax.cond(case[0] == len(cases) - 1, functools.partial(move, ((lo,) * nch,), False, 2),
                       functools.partial(move, ((0,) * nch,), False, 2), *slo)
        yownl, yownh = ffn('own', hb, ((0, light), (0, heavy)), light + heavy, [ownl, ownh])
        held = lax.optimization_barrier((yownl, *xlb))
        yownl, xlb = held[0], held[1:]
        yl = ffn('light', lb, far(light), light, pairs(xlb, xlo))
        ylb, ylo = yl[::2], yl[1::2]
        held = lax.optimization_barrier((*sho, *ylb))
        xho, = choose(lambda n, c: (c,), False, 0, held[:nk])
        held = lax.optimization_barrier((*ylb, *xho))
        ylb, xho = held[:nk], held[nk:]
        zlb = [shift(ylb[k], nch - 1 - k) for k in range(nk)]
        yh = ffn('heavy', hb, far(heavy), heavy, pairs(xhb, xho))
        yhb, yho = yh[::2], yh[1::2]
        zhb, zho, zlo = choose(lambda n, c: ((hb,) * nch, c, lights(n)), True, 1, [*yhb, *yho, *ylo])

        return pl.pallas_call(
            functools.partial(_unpack_kernel, nch, bases),
            out_shape=sds((tok, d), bf),
            in_specs=[SMEM] * 4 + [ANY] * (2 + 4 * nk), out_specs=ANY,
            scratch_shapes=[pltpu.VMEM((rows, d), bf), pltpu.VMEM((rows * nl, 128), jnp.float32),
                            pltpu.VMEM((tok * nl, 128), jnp.float32), pltpu.VMEM((tok, d), bf),
                            pltpu.SemaphoreType.DMA((nch,)), pltpu.SemaphoreType.DMA((CHUNKS,))],
            compiler_params=params, name='unpack',
        )(cnt, me, pos, wt, yownl, yownh, *[v for p in zip(zlb, zlo, zhb, zho) for v in p])

    return jax.shard_map(local, mesh=mesh, in_specs=(tok_spec,) * 5 + (w_spec,) * 3,
                         out_specs=tok_spec, check_vma=False)
```
